256 devices in a mesh: space: 64 (over y, z, core), col: 4 (over x).
Axes of the slice: x: 4, y: 4, z: 8, core: 2. Of those that a mesh axis runs over, the one named last changes fastest.
Arguments:
- first_snaps: float32 [458752, 512], P(('space', 'col')), may hold values from -7200 to 7200, as said below
- next_snaps: float32 [458752, 512], P(('space', 'col')), may hold values from -24 to 24
Outputs:
- reduced_operator: float32 [512, 512], replicated
- mode_basis: float32 [458752, 512], P(('space', 'col'))
The draws below stay inside these ranges and needn't reach their ends.
Inputs may be any that keep to these rules, and one draw needn't show every extreme that they name: `first_snaps`: Real-valued snapshots; the columns are linearly independent.
All inputs are finite; a program needn't handle non-finite values.
Results may differ from the reference program's by a relative error of at most 0.00017.
Values sent between devices are 32-bit elements; how exact they have to be, the bound alone decides.
A program may use at most 64 MiB of HBM per device.

```python
import math
import jax
import jax.numpy as jnp
from jax import lax

K = 512
ROWS_DEV = 1792
ROWS = 458752
BLOCKS = 256


def draw_first_snaps(key, part):
    keys = jax.random.split(key, 8)
    base = jax.random.normal(keys[0], (ROWS, K), jnp.float32)
    base = jnp.clip(base, -6.0, 6.0)
    positions = jnp.arange(ROWS, dtype=jnp.float32)
    row_scale = jnp.exp(jax.random.uniform(keys[1], (ROWS, 1), jnp.float32, 0.0, math.log(10.0)))
    row_scale = row_scale * jnp.exp(math.log(3.0) * positions / ROWS)[:, None]
    col_scale = jnp.exp(jax.random.uniform(keys[2], (1, K), jnp.float32, 0.0, math.log(10.0)))
    order = jax.random.permutation(keys[3], BLOCKS)
    width = max(K // BLOCKS, 1)
    row_block = jnp.arange(ROWS, dtype=jnp.int32) // ROWS_DEV
    start = order[row_block] * width % K
    column = jnp.arange(K, dtype=jnp.int32)
    inside = (column[None, :] >= start[:, None]) & (column[None, :] < start[:, None] + width)
    factor = jnp.where(inside, 4.0, 1.0)
    result = (base * row_scale * col_scale * factor).astype(jnp.float32)
    spots = jax.random.randint(keys[6], (2,), 0, ROWS // 2)
    cols = jax.random.randint(keys[7], (2,), 0, K // 2)
    result = result.at[spots[0], cols[0]].set(7200.0)
    result = result.at[spots[1] + ROWS // 2, cols[1] + K // 2].set(-7200.0)
    return result


def with_spikes(drawn, stream_key, source, target, shards_of, factor):
    owner, partner = [(jnp.arange(drawn.shape[axis_at]) // (drawn.shape[axis_at] // shards_of)).reshape([-1 if axis == axis_at else 1 for axis in range(drawn.ndim)]) for axis_at in (source, target)]
    chosen = jax.random.permutation(stream_key, shards_of)[partner]
    strong = (owner == chosen) | (owner == (partner + shards_of // 2) % shards_of)
    return jnp.where(strong, factor * drawn, drawn)


def steps_of(key, shape, pieces, smallest, top_value):
    loudness, own = 1.0, jax.random.fold_in(key, 6)
    for axis_at, shards_of in pieces:
        heights = jnp.exp(jax.random.uniform(jax.random.fold_in(own, axis_at), (shards_of,), jnp.float32, smallest / len(pieces), top_value / len(pieces)))
        loudness = loudness * jnp.repeat(heights, shape[axis_at] // shards_of).reshape([-1 if axis == axis_at else 1 for axis in range(len(shape))])
    return loudness


def noise_with(key, extent, scale, reach, shards, heavy, kind=jnp.bfloat16):
    values = scale * jax.random.normal(key, extent, jnp.float32)
    if shards:
        values = values * steps_of(key, extent, shards, -0.22, 0.18)
    return jnp.clip(with_spikes(values, jax.random.fold_in(key, 3), *heavy), -reach, reach).astype(kind)


def setup_inputs(seed: int = 0) -> dict:
    seeds = jax.random.split(jax.random.key(seed), 3)
    first_snaps = draw_first_snaps(jax.random.fold_in(seeds[2], 71), 0)
    next_snaps = noise_with(seeds[1], (ROWS, K), 1.0, 24.0, ((0, 256),), (0, 1, 256, 6.0), jnp.float32)
    return {"first_snaps": first_snaps, "next_snaps": next_snaps}


def reference(first_snaps, next_snaps):
    highest = lax.Precision.HIGHEST
    dims = (((0,), (0,)), ((), ()))
    gram = lax.dot_general(first_snaps.astype(jnp.float32), first_snaps.astype(jnp.float32), dims, precision=highest, preferred_element_type=jnp.float32)
    cross = lax.dot_general(first_snaps.astype(jnp.float32), next_snaps.astype(jnp.float32), dims, precision=highest, preferred_element_type=jnp.float32)
    lower = jnp.linalg.cholesky(gram)
    scale = math.sqrt(ROWS)
    left = jax.scipy.linalg.solve_triangular(lower, cross, lower=True)
    reduced_operator = jax.scipy.linalg.solve_triangular(lower, left.T, lower=True).T * scale
    mode_basis = jax.scipy.linalg.solve_triangular(lower, next_snaps.T, lower=True).T * scale
    return (reduced_operator, mode_basis)
```

```python
import functools
import math

import jax
import jax.numpy as jnp
from jax import lax
from jax.experimental import pallas as pl
from jax.experimental.pallas import tpu as pltpu
from jax.sharding import Mesh
from jax.sharding import PartitionSpec as P

AXES = ("y", "z", "c", "x")
MESH = pl.DeviceIdType.MESH
K = 512
NB = 128
F32, BF16 = jnp.float32, jnp.bfloat16
T0 = (((0,), (0,)), ((), ()))
NN = (((1,), (0,)), ((), ()))
NT = (((1,), (1,)), ((), ()))
UPPER = [(i, j) for i in range(4) for j in range(i, 4)]


def split2(x):
    hi = x.astype(BF16)
    return hi, (x - hi.astype(F32)).astype(BF16)


def split3(x):
    hi = x.astype(BF16)
    rest = x - hi.astype(F32)
    mid = rest.astype(BF16)
    return hi, mid, (rest - mid.astype(F32)).astype(BF16)


def mm(a, b, dims):
    return lax.dot_general(a, b, dims, preferred_element_type=F32)


def lane_splat(v, lane):
    return jnp.broadcast_to(v[:, lane : lane + 1], v.shape)


def row_splat(v, row):
    return jnp.broadcast_to(v[row : row + 1, :], v.shape)


def eliminate_block(w, out):
    sub = lax.broadcasted_iota(jnp.int32, (8, NB), 0)
    for t in range(NB // 8):
        r0 = 8 * t
        pa, pb = w[r0 : r0 + 8, :NB], w[r0 : r0 + 8, NB:]
        s = [lane_splat(pa, r0 + j) for j in range(8)]
        rs, uas, ubs, ums = [], [], [], []
        for j in range(8):
            r = lax.rsqrt(row_splat(s[j], j))
            low = jnp.where(sub > j, s[j] * r, 0.0)
            ua, ub = row_splat(pa, j) * r, row_splat(pb, j) * r
            um = {m: row_splat(s[m], j) * r for m in range(j + 1, 8)}
            for m in um:
                s[m] = s[m] - low * um[m]
            pa, pb = pa - low * ua, pb - low * ub
            out[r0 + j : r0 + j + 1, :] = ub[0:1, :]
            rs.append(r), uas.append(ua), ubs.append(ub), ums.append(um)
        for g in range(t + 1, NB // 8):
            rows = slice(8 * g, 8 * g + 8)
            wa, wb = w[rows, :NB], w[rows, NB:]
            sg = [lane_splat(wa, r0 + j) for j in range(8)]
            for j in range(8):
                low = sg[j] * rs[j]
                for m in range(j + 1, 8):
                    sg[m] = sg[m] - low * ums[j][m]
                wa, wb = wa - low * uas[j], wb - low * ubs[j]
            w[rows, :NB], w[rows, NB:] = wa, wb


def dot6(a3, b3, dims):
    ca, cb = dims[0][0][0], dims[0][1][0]
    ah, am, al = a3
    bh, bm, bl = b3
    left = jnp.concatenate([ah, ah, am, ah, al, am], axis=ca)
    right = jnp.concatenate([bh, bm, bh, bl, bh, bm], axis=cb)
    return mm(left, right, dims)


def invert_factor(z, w, m11, m):
    eye = jnp.where(
        lax.broadcasted_iota(jnp.int32, (NB, NB), 0) == lax.broadcasted_iota(jnp.int32, (NB, NB), 1), 1.0, 0.0
    ).astype(F32)
    for kb in range(4):
        c0, c1 = kb * NB, (kb + 1) * NB
        rows = slice(c0, c1)
        w[:, :NB] = z[rows, c0:c1]
        w[:, NB:] = eye
        eliminate_block(w, m11)
        inv = m11[...]
        m[rows, c0:c1] = inv
        inv3 = split3(inv)
        if kb > 0:
            left = dot6(inv3, split3(z[rows, :c0]), NN)
            m[rows, :c0] = left
            left3 = split3(left)
        if kb < 3:
            m[rows, c1:] = jnp.zeros((NB, K - c1), F32)
            right3 = split3(dot6(inv3, split3(z[rows, c1:]), NN))
            z[c1:, c1:] = z[c1:, c1:] - dot6(right3, right3, T0)
            z[c1:, c0:c1] = -dot6(right3, inv3, T0)
            if kb > 0:
                z[c1:, :c0] = z[c1:, :c0] - dot6(right3, left3, T0)


def finish_kernel(scale, g_ref, c_ref, y_ref, red_ref, mode_ref, z, w, m11, m, mh, ml):
    @pl.when(pl.program_id(0) == 0)
    def _():
        for b, (i, j) in enumerate(UPPER):
            z[i * NB : (i + 1) * NB, j * NB : (j + 1) * NB] = g_ref[b // 5, (b % 5) * NB : (b % 5 + 1) * NB, :]
        invert_factor(z, w, m11, m)
        hi, lo = split2(m[...])
        mh[...], ml[...] = hi, lo
        for b in range(16):
            i, j = b // 4, b % 4
            z[i * NB : (i + 1) * NB, j * NB : (j + 1) * NB] = c_ref[b // 8, (b % 8) * NB : (b % 8 + 1) * NB, :]
        ch, cl = split2(z[...])
        lh, ll = split2(mm(hi, ch, NN) + mm(hi, cl, NN) + mm(lo, ch, NN))
        red_ref[...] = (mm(lh, hi, NT) + mm(lh, lo, NT) + mm(ll, hi, NT)) * scale

    yh, yl = split2(y_ref[...])
    for n, k1 in ((0, 256), (256, 512)):
        ph, plo = mh[n : n + 256, :k1], ml[n : n + 256, :k1]
        ah, al = yh[:, :k1], yl[:, :k1]
        mode_ref[:, n : n + 256] = (mm(ah, ph, NT) + mm(ah, plo, NT) + mm(al, ph, NT)) * scale


def finish(gram, cross, y, scale):
    rows = y.shape[0]
    step = rows // 4
    whole = lambda *shape: pl.BlockSpec(shape, lambda i: (0,) * len(shape))
    return pl.pallas_call(
        functools.partial(finish_kernel, scale),
        grid=(4,),
        out_shape=(jax.ShapeDtypeStruct((K, K), F32), jax.ShapeDtypeStruct((rows, K), F32)),
        in_specs=[whole(*gram.shape), whole(*cross.shape), pl.BlockSpec((step, K), lambda i: (i, 0))],
        out_specs=(whole(K, K), pl.BlockSpec((step, K), lambda i: (i, 0))),
        scratch_shapes=[
            pltpu.VMEM((K, K), F32),
            pltpu.VMEM((NB, 2 * NB), F32),
            pltpu.VMEM((NB, NB), F32),
            pltpu.VMEM((K, K), F32),
            pltpu.VMEM((K, K), BF16),
            pltpu.VMEM((K, K), BF16),
        ],
        compiler_params=pltpu.CompilerParams(vmem_limit_bytes=60 << 20),
        name="factor_and_modes",
    )(gram, cross, y)


GP, CP = 40, 64


def to_blocks(ref, first, value):
    per = ref.shape[1] // NB
    for n in range(value.shape[1] // NB):
        b = first + n
        ref[b // per, (b % per) * NB : (b % per + 1) * NB, :] = value[:, n * NB : (n + 1) * NB]


def sums_kernel(x_hbm, y_hbm, g_out, c_out, xv, yv, xh, xl, yh, yl, gloc, cloc, gpart, cpart, gsum, csum, gxy, cxy, gz, cz,
                gred, in_sem, d_send, d_recv, xy_send, xy_recv, z_send, z_recv, ag_send, ag_recv, e_send, e_recv, c_sem):
    my, mz, mc, mx = [lax.axis_index(a) for a in AXES]
    oc = 1 - mc
    me = my * 4 + mx
    rows = xv.shape[0]
    chunks = rows // 256

    loads = []
    for n, (src, dst) in enumerate(((x_hbm, xv), (y_hbm, yv))):
        for i in range(chunks):
            part = pl.ds(i * 256, 256)
            loads.append(pltpu.make_async_copy(src.at[part], dst.at[part], in_sem.at[n * chunks + i]))
    for load in loads:
        load.start()

    plane = [(dy, dx) for dy in range(4) for dx in range(4)][1:]

    def in_plane(dy, dx):
        return lax.rem(my + dy, 4), lax.rem(mx + dx, 4)

    def along_z(dz):
        return lax.rem(mz + dz, 8)

    barrier = pltpu.get_barrier_semaphore()
    pl.semaphore_signal(barrier, inc=1, device_id=(my, mz, oc, mx), device_id_type=MESH)
    for dy, dx in plane:
        py, px = in_plane(dy, dx)
        pl.semaphore_signal(barrier, inc=1, device_id=(py, mz, mc, px), device_id_type=MESH)
    for dz in range(1, 8):
        pl.semaphore_signal(barrier, inc=1, device_id=(my, along_z(dz), mc, mx), device_id_type=MESH)

    def partner(src, dst, n, sems):
        return pltpu.make_async_remote_copy(src, dst, sems[0].at[n], sems[1].at[n], device_id=(my, mz, oc, mx), device_id_type=MESH)

    def piece(ref, who, size):
        return ref.at[pl.ds(pl.multiple_of(who * size, 8), size), :]

    def scatter_plane(part, landing, size, n):
        out = []
        for k, (dy, dx) in enumerate(plane):
            py, px = in_plane(dy, dx)
            out.append(pltpu.make_async_remote_copy(
                piece(part, py * 4 + px, size), landing.at[k], xy_send.at[n, k], xy_recv.at[n, k],
                device_id=(py, mz, mc, px), device_id_type=MESH))
        return out

    def gather_plane(mine, whole, size, n):
        out = []
        for k, (dy, dx) in enumerate(plane):
            py, px = in_plane(dy, dx)
            out.append(pltpu.make_async_remote_copy(
                mine, piece(whole, me, size), ag_send.at[n, k], ag_recv.at[n, k],
                device_id=(py, mz, mc, px), device_id_type=MESH))
        return out

    def start(copies):
        for c in copies:
            c.start()

    def wait(copies):
        for c in copies:
            c.wait()

    for i in range(chunks):
        loads[i].wait()
        part = slice(i * 256, i * 256 + 256)
        xh[part, :], xl[part, :] = split2(xv[part, :])
    left, right = slice(0, 256), slice(256, 512)
    for cols, firsts in ((left, (0, 4)), (right, (7, 9))):
        h, l = xh[:, cols], xl[:, cols]
        hl = mm(h, l, T0)
        g = mm(h, h, T0) + mm(l, l, T0) + hl + hl.T
        to_blocks(gloc, firsts[0], g[:NB])
        to_blocks(gloc, firsts[1], g[NB:, NB:])
    h, l = xh[:, left], xl[:, left]
    h2, l2 = xh[:, right], xl[:, right]
    g = mm(h, h2, T0) + mm(h, l2, T0) + mm(l, h2, T0) + mm(l, l2, T0)
    to_blocks(gloc, 2, g[:NB])
    to_blocks(gloc, 5, g[NB:])

    pl.semaphore_wait(barrier, 1 + len(plane) + 7)
    g_d = partner(gloc.at[oc], gpart, 0, (d_send, d_recv))
    g_d.start()

    for i in range(chunks):
        loads[chunks + i].wait()
        part = slice(i * 256, i * 256 + 256)
        yh[part, :], yl[part, :] = split2(yv[part, :])
    for i in range(4):
        h, l = xh[:, i * NB : (i + 1) * NB], xl[:, i * NB : (i + 1) * NB]
        to_blocks(cloc, 4 * i, mm(h, yh[...], T0) + mm(h, yl[...], T0) + mm(l, yh[...], T0))
    c_d = partner(cloc.at[oc], cpart, 1, (d_send, d_recv))
    c_d.start()

    g_d.wait()
    gsum[...] = gloc[mc] + gpart[...]
    g_xy = scatter_plane(gsum, gxy, GP, 0)
    start(g_xy)
    c_d.wait()
    csum[...] = cloc[mc] + cpart[...]
    c_xy = scatter_plane(csum, cxy, CP, 1)
    start(c_xy)

    wait(g_xy)
    total = gsum[pl.ds(pl.multiple_of(me * GP, 8), GP), :]
    for k in range(15):
        total = total + gxy[k]
    gred[...] = total
    gz[mz] = total
    g_z = [pltpu.make_async_remote_copy(gred, gz.at[mz], z_send.at[0, k], z_recv.at[0, k],
                                        device_id=(my, along_z(k + 1), mc, mx), device_id_type=MESH) for k in range(7)]
    start(g_z)

    wait(c_xy)
    total = csum[pl.ds(pl.multiple_of(me * CP, 8), CP), :]
    for k in range(15):
        total = total + cxy[k]
    csum[0:CP, :] = total
    c_z = [pltpu.make_async_remote_copy(piece(csum, along_z(k + 1), 8), cz.at[k], z_send.at[1, k], z_recv.at[1, k],
                                        device_id=(my, along_z(k + 1), mc, mx), device_id_type=MESH) for k in range(7)]
    start(c_z)

    wait(g_z)
    total = gz[0]
    for k in range(1, 8):
        total = total + gz[k]
    g_out[mc, pl.ds(pl.multiple_of(me * GP, 8), GP), :] = total
    g_ag = gather_plane(piece(g_out.at[mc], me, GP), g_out.at[mc], GP, 0)
    start(g_ag)

    wait(c_z)
    total = csum[pl.ds(pl.multiple_of(mz * 8, 8), 8), :]
    for k in range(7):
        total = total + cz[k]
    mine = pl.multiple_of(me * CP, 8)
    c_out[mc, pl.ds(mine + pl.multiple_of(mz * 8, 8), 8), :] = total
    src = c_out.at[mc, pl.ds(mine + pl.multiple_of(mz * 8, 8), 8), :]
    c_zg = [pltpu.make_async_remote_copy(src, src, z_send.at[2, k], z_recv.at[2, k],
                                         device_id=(my, along_z(k + 1), mc, mx), device_id_type=MESH) for k in range(7)]
    start(c_zg)

    wait(g_ag)
    g_e = partner(g_out.at[mc], g_out.at[mc], 0, (e_send, e_recv))
    g_e.start()

    wait(c_zg)
    c_ag = gather_plane(piece(c_out.at[mc], me, CP), c_out.at[mc], CP, 1)
    start(c_ag)
    wait(c_ag)
    c_e = partner(c_out.at[mc], c_out.at[mc], 1, (e_send, e_recv))
    c_e.start()
    g_e.wait()
    c_e.wait()


def sums(x, y):
    rows = x.shape[0]
    chunks = rows // 256
    vm = pltpu.VMEM
    dma = pltpu.SemaphoreType.DMA
    return pl.pallas_call(
        sums_kernel,
        out_shape=(jax.ShapeDtypeStruct((2, 640, NB), F32), jax.ShapeDtypeStruct((2, 1024, NB), F32)),
        in_specs=[pl.BlockSpec(memory_space=pl.ANY)] * 2,
        out_specs=(pl.BlockSpec(memory_space=pltpu.VMEM),) * 2,
        scratch_shapes=[
            vm((rows, K), F32), vm((rows, K), F32),
            vm((rows, K), BF16), vm((rows, K), BF16), vm((rows, K), BF16), vm((rows, K), BF16),
            vm((2, 640, NB), F32), vm((2, 1024, NB), F32),
            vm((640, NB), F32), vm((1024, NB), F32), vm((640, NB), F32), vm((1024, NB), F32),
            vm((15, GP, NB), F32), vm((15, CP, NB), F32), vm((8, GP, NB), F32), vm((7, 8, NB), F32), vm((GP, NB), F32),
            dma((2 * chunks,)), dma((2,)), dma((2,)), dma((2, 15)), dma((2, 15)), dma((3, 7)), dma((3, 7)),
            dma((2, 15)), dma((2, 15)), dma((2,)), dma((2,)), dma(()),
        ],
        compiler_params=pltpu.CompilerParams(collective_id=0, has_side_effects=True, vmem_limit_bytes=60 << 20),
        name="products_and_sums",
    )(x, y)


def on_device(first_snaps, next_snaps):
    scale = math.sqrt(first_snaps.shape[0] * lax.axis_size(AXES))
    gram, cross = sums(first_snaps, next_snaps)
    return finish(gram, cross, next_snaps, scale)


def solution(mesh):
    finer = Mesh(mesh.devices.reshape(4, 8, 2, 4), AXES)
    spec = P(AXES, None)
    return jax.shard_map(
        on_device, mesh=finer, in_specs=(spec, spec), out_specs=(P(), spec), check_vma=False
    )
```

```python
import functools
import math

import jax
import jax.numpy as jnp
from jax import lax
from jax.experimental import pallas as pl
from jax.experimental.pallas import tpu as pltpu
from jax.sharding import Mesh
from jax.sharding import PartitionSpec as P

AXES = ("y", "z", "c", "x")
MESH = pl.DeviceIdType.MESH
K = 512
NB = 128
F32, BF16 = jnp.float32, jnp.bfloat16
T0 = (((0,), (0,)), ((), ()))
NN = (((1,), (0,)), ((), ()))
NT = (((1,), (1,)), ((), ()))
UPPER = [(i, j) for i in range(4) for j in range(i, 4)]


def split2(x):
    hi = x.astype(BF16)
    return hi, (x - hi.astype(F32)).astype(BF16)


def split3(x):
    hi = x.astype(BF16)
    rest = x - hi.astype(F32)
    mid = rest.astype(BF16)
    return hi, mid, (rest - mid.astype(F32)).astype(BF16)


def mm(a, b, dims):
    return lax.dot_general(a, b, dims, preferred_element_type=F32)


def lane_splat(v, lane):
    return jnp.broadcast_to(v[:, lane : lane + 1], v.shape)


def row_splat(v, row):
    return jnp.broadcast_to(v[row : row + 1, :], v.shape)


def eliminate_block(w, out):
    sub = lax.broadcasted_iota(jnp.int32, (8, NB), 0)
    for t in range(NB // 8):
        r0 = 8 * t
        pa, pb = w[r0 : r0 + 8, :NB], w[r0 : r0 + 8, NB:]
        s = [lane_splat(pa, r0 + j) for j in range(8)]
        rs, uas, ubs, ums = [], [], [], []
        for j in range(8):
            r = lax.rsqrt(row_splat(s[j], j))
            low = jnp.where(sub > j, s[j] * r, 0.0)
            ua, ub = row_splat(pa, j) * r, row_splat(pb, j) * r
            um = {m: row_splat(s[m], j) * r for m in range(j + 1, 8)}
            for m in um:
                s[m] = s[m] - low * um[m]
            pa, pb = pa - low * ua, pb - low * ub
            out[r0 + j : r0 + j + 1, :] = ub[0:1, :]
            rs.append(r), uas.append(ua), ubs.append(ub), ums.append(um)
        for g in range(t + 1, NB // 8):
            rows = slice(8 * g, 8 * g + 8)
            wa, wb = w[rows, :NB], w[rows, NB:]
            sg = [lane_splat(wa, r0 + j) for j in range(8)]
            for j in range(8):
                low = sg[j] * rs[j]
                for m in range(j + 1, 8):
                    sg[m] = sg[m] - low * ums[j][m]
                wa, wb = wa - low * uas[j], wb - low * ubs[j]
            w[rows, :NB], w[rows, NB:] = wa, wb


def dot6(a3, b3, dims):
    ca, cb = dims[0][0][0], dims[0][1][0]
    ah, am, al = a3
    bh, bm, bl = b3
    left = jnp.concatenate([ah, ah, am, ah, al, am], axis=ca)
    right = jnp.concatenate([bh, bm, bh, bl, bh, bm], axis=cb)
    return mm(left, right, dims)


def invert_factor(z, w, m11, m, between):
    eye = jnp.where(
        lax.broadcasted_iota(jnp.int32, (NB, NB), 0) == lax.broadcasted_iota(jnp.int32, (NB, NB), 1), 1.0, 0.0
    ).astype(F32)
    cols = lax.broadcasted_iota(jnp.int32, (NB, K), 1)
    wide = lax.broadcasted_iota(jnp.int32, (K, K), 1)

    def block_step(kb, carry):
        between(kb)
        c0 = pl.multiple_of(kb * NB, NB)
        c1 = c0 + NB
        rows = pl.ds(c0, NB)
        w[:, :NB] = z[rows, rows]
        w[:, NB:] = eye
        eliminate_block(w, m11)
        z[rows, rows] = eye
        t = dot6(split3(m11[...]), split3(z[rows, :]), NN)
        m[rows, :] = jnp.where(cols < c1, t, 0.0)
        later = cols >= c1
        t3 = split3(t)
        update = dot6(split3(jnp.where(later, t, 0.0)), t3, T0)
        z[...] = jnp.where((wide >= c0) & (wide < c1), 0.0, z[...]) - update
        return carry

    lax.fori_loop(0, K // NB, block_step, 0)


def finish_kernel(scale, m_ref, c_ref, y_ref, red_ref, mode_ref, z, mh, ml):
    @pl.when(pl.program_id(0) == 0)
    def _():
        hi, lo = split2(m_ref[...])
        mh[...], ml[...] = hi, lo
        for b in range(16):
            i, j = b // 4, b % 4
            z[i * NB : (i + 1) * NB, j * NB : (j + 1) * NB] = c_ref[b // 8, (b % 8) * NB : (b % 8 + 1) * NB, :]
        ch, cl = split2(z[...])
        lh, ll = split2(mm(hi, ch, NN) + mm(hi, cl, NN) + mm(lo, ch, NN))
        red_ref[...] = (mm(lh, hi, NT) + mm(lh, lo, NT) + mm(ll, hi, NT)) * scale

    yh, yl = split2(y_ref[...])
    for n, k1 in ((0, 256), (256, 512)):
        ph, plo = mh[n : n + 256, :k1], ml[n : n + 256, :k1]
        ah, al = yh[:, :k1], yl[:, :k1]
        mode_ref[:, n : n + 256] = (mm(ah, ph, NT) + mm(ah, plo, NT) + mm(al, ph, NT)) * scale


def finish(m, cross, y, scale):
    rows = y.shape[0]
    step = rows // 4
    whole = lambda *shape: pl.BlockSpec(shape, lambda i: (0,) * len(shape))
    return pl.pallas_call(
        functools.partial(finish_kernel, scale),
        grid=(4,),
        out_shape=(jax.ShapeDtypeStruct((K, K), F32), jax.ShapeDtypeStruct((rows, K), F32)),
        in_specs=[whole(K, K), whole(*cross.shape), pl.BlockSpec((step, K), lambda i: (i, 0))],
        out_specs=(whole(K, K), pl.BlockSpec((step, K), lambda i: (i, 0))),
        scratch_shapes=[pltpu.VMEM((K, K), F32), pltpu.VMEM((K, K), BF16), pltpu.VMEM((K, K), BF16)],
        compiler_params=pltpu.CompilerParams(vmem_limit_bytes=60 << 20),
        name="operator_and_modes",
    )(m, cross, y)


GP, CP = 40, 64


def to_blocks(ref, first, value):
    per = ref.shape[1] // NB
    for n in range(value.shape[1] // NB):
        b = first + n
        ref[b // per, (b % per) * NB : (b % per + 1) * NB, :] = value[:, n * NB : (n + 1) * NB]


def sums_kernel(x_hbm, y_hbm, m_out, c_out, g_out, z, w, m11, xv, yv, xh, xl, yh, yl, gloc, cloc, gpart, cpart, gsum, csum, gxy, cxy, gz, cz,
                gred, in_sem, d_send, d_recv, xy_send, xy_recv, z_send, z_recv, ag_send, ag_recv, e_send, e_recv):
    my, mz, mc, mx = [lax.axis_index(a) for a in AXES]
    oc = 1 - mc
    me = my * 4 + mx
    rows = xv.shape[0]
    chunks = rows // 256

    loads = []
    for n, (src, dst) in enumerate(((x_hbm, xv), (y_hbm, yv))):
        for i in range(chunks):
            part = pl.ds(i * 256, 256)
            loads.append(pltpu.make_async_copy(src.at[part], dst.at[part], in_sem.at[n * chunks + i]))
    for load in loads:
        load.start()

    plane = [(dy, dx) for dy in range(4) for dx in range(4)][1:]

    def in_plane(dy, dx):
        return lax.rem(my + dy, 4), lax.rem(mx + dx, 4)

    def along_z(dz):
        return lax.rem(mz + dz, 8)

    barrier = pltpu.get_barrier_semaphore()
    pl.semaphore_signal(barrier, inc=1, device_id=(my, mz, oc, mx), device_id_type=MESH)
    for dy, dx in plane:
        py, px = in_plane(dy, dx)
        pl.semaphore_signal(barrier, inc=1, device_id=(py, mz, mc, px), device_id_type=MESH)
    for dz in range(1, 8):
        pl.semaphore_signal(barrier, inc=1, device_id=(my, along_z(dz), mc, mx), device_id_type=MESH)

    def partner(src, dst, n, sems):
        return pltpu.make_async_remote_copy(src, dst, sems[0].at[n], sems[1].at[n], device_id=(my, mz, oc, mx), device_id_type=MESH)

    def piece(ref, who, size):
        return ref.at[pl.ds(pl.multiple_of(who * size, 8), size), :]

    def scatter_plane(part, landing, size, n):
        out = []
        for k, (dy, dx) in enumerate(plane):
            py, px = in_plane(dy, dx)
            out.append(pltpu.make_async_remote_copy(
                piece(part, py * 4 + px, size), landing.at[k], xy_send.at[n, k], xy_recv.at[n, k],
                device_id=(py, mz, mc, px), device_id_type=MESH))
        return out

    def gather_plane(mine, whole, size, n):
        out = []
        for k, (dy, dx) in enumerate(plane):
            py, px = in_plane(dy, dx)
            out.append(pltpu.make_async_remote_copy(
                mine, piece(whole, me, size), ag_send.at[n, k], ag_recv.at[n, k],
                device_id=(py, mz, mc, px), device_id_type=MESH))
        return out

    def start(copies):
        for c in copies:
            c.start()

    def wait(copies):
        for c in copies:
            c.wait()

    for i in range(chunks):
        loads[i].wait()
        part = slice(i * 256, i * 256 + 256)
        xh[part, :], xl[part, :] = split2(xv[part, :])
    left, right = slice(0, 256), slice(256, 512)
    for cols, firsts in ((left, (0, 4)), (right, (7, 9))):
        h, l = xh[:, cols], xl[:, cols]
        hl = mm(h, l, T0)
        g = mm(h, h, T0) + mm(l, l, T0) + hl + hl.T
        to_blocks(gloc, firsts[0], g[:NB])
        to_blocks(gloc, firsts[1], g[NB:, NB:])
    h, l = xh[:, left], xl[:, left]
    h2, l2 = xh[:, right], xl[:, right]
    g = mm(h, h2, T0) + mm(h, l2, T0) + mm(l, h2, T0) + mm(l, l2, T0)
    to_blocks(gloc, 2, g[:NB])
    to_blocks(gloc, 5, g[NB:])

    pl.semaphore_wait(barrier, 1 + len(plane) + 7)
    g_d = partner(gloc.at[oc], gpart, 0, (d_send, d_recv))
    g_d.start()

    for i in range(chunks):
        loads[chunks + i].wait()
        part = slice(i * 256, i * 256 + 256)
        yh[part, :], yl[part, :] = split2(yv[part, :])

    def cross_band(i):
        h, l = xh[:, i * NB : (i + 1) * NB], xl[:, i * NB : (i + 1) * NB]
        to_blocks(cloc, 4 * i, mm(h, yh[...], T0) + mm(h, yl[...], T0) + mm(l, yh[...], T0))

    cross_band(0)

    g_d.wait()
    gsum[...] = gloc[mc] + gpart[...]
    g_xy = scatter_plane(gsum, gxy, GP, 0)
    start(g_xy)
    cross_band(1)
    cross_band(2)
    cross_band(3)
    c_d = partner(cloc.at[oc], cpart, 1, (d_send, d_recv))
    c_d.start()
    c_d.wait()
    csum[...] = cloc[mc] + cpart[...]
    c_xy = scatter_plane(csum, cxy, CP, 1)
    start(c_xy)

    wait(g_xy)
    total = gsum[pl.ds(pl.multiple_of(me * GP, 8), GP), :]
    for k in range(15):
        total = total + gxy[k]
    gred[...] = total
    gz[mz] = total
    g_z = [pltpu.make_async_remote_copy(gred, gz.at[mz], z_send.at[0, k], z_recv.at[0, k],
                                        device_id=(my, along_z(k + 1), mc, mx), device_id_type=MESH) for k in range(7)]
    start(g_z)

    wait(g_z)
    total = gz[0]
    for k in range(1, 8):
        total = total + gz[k]
    g_out[mc, pl.ds(pl.multiple_of(me * GP, 8), GP), :] = total
    g_ag = gather_plane(piece(g_out.at[mc], me, GP), g_out.at[mc], GP, 0)
    start(g_ag)

    wait(c_xy)
    total = csum[pl.ds(pl.multiple_of(me * CP, 8), CP), :]
    for k in range(15):
        total = total + cxy[k]
    csum[0:CP, :] = total
    c_z = [pltpu.make_async_remote_copy(piece(csum, along_z(k + 1), 8), cz.at[k], z_send.at[1, k], z_recv.at[1, k],
                                        device_id=(my, along_z(k + 1), mc, mx), device_id_type=MESH) for k in range(7)]
    start(c_z)

    wait(g_ag)
    g_e = partner(g_out.at[mc], g_out.at[mc], 0, (e_send, e_recv))
    g_e.start()

    wait(c_z)
    total = csum[pl.ds(pl.multiple_of(mz * 8, 8), 8), :]
    for k in range(7):
        total = total + cz[k]
    own = pl.ds(pl.multiple_of(me * CP + mz * 8, 8), 8)
    c_out[mc, own, :] = total
    c_zg = [pltpu.make_async_remote_copy(c_out.at[mc, own, :], c_out.at[mc, own, :], z_send.at[2, k], z_recv.at[2, k],
                                         device_id=(my, along_z(k + 1), mc, mx), device_id_type=MESH) for k in range(7)]
    start(c_zg)
    c_ag = gather_plane(piece(c_out.at[mc], me, CP), c_out.at[mc], CP, 1)
    c_e = partner(c_out.at[mc], c_out.at[mc], 1, (e_send, e_recv))

    def between(kb):
        @pl.when(kb == 1)
        def _():
            wait(c_zg)
            start(c_ag)

        @pl.when(kb == 3)
        def _():
            wait(c_ag)
            c_e.start()

    g_e.wait()
    for b, (i, j) in enumerate(UPPER):
        z[i * NB : (i + 1) * NB, j * NB : (j + 1) * NB] = g_out[b // 5, (b % 5) * NB : (b % 5 + 1) * NB, :]
    invert_factor(z, w, m11, m_out, between)
    c_e.wait()


def sums(x, y):
    rows = x.shape[0]
    chunks = rows // 256
    vm = pltpu.VMEM
    dma = pltpu.SemaphoreType.DMA
    return pl.pallas_call(
        sums_kernel,
        out_shape=(jax.ShapeDtypeStruct((K, K), F32), jax.ShapeDtypeStruct((2, 1024, NB), F32)),
        in_specs=[pl.BlockSpec(memory_space=pl.ANY)] * 2,
        out_specs=(pl.BlockSpec(memory_space=pltpu.VMEM),) * 2,
        scratch_shapes=[
            vm((2, 640, NB), F32), vm((K, K), F32), vm((NB, 2 * NB), F32), vm((NB, NB), F32),
            vm((rows, K), F32), vm((rows, K), F32),
            vm((rows, K), BF16), vm((rows, K), BF16), vm((rows, K), BF16), vm((rows, K), BF16),
            vm((2, 640, NB), F32), vm((2, 1024, NB), F32),
            vm((640, NB), F32), vm((1024, NB), F32), vm((640, NB), F32), vm((1024, NB), F32),
            vm((15, GP, NB), F32), vm((15, CP, NB), F32), vm((8, GP, NB), F32), vm((7, 8, NB), F32), vm((GP, NB), F32),
            dma((2 * chunks,)), dma((2,)), dma((2,)), dma((2, 15)), dma((2, 15)), dma((3, 7)), dma((3, 7)),
            dma((2, 15)), dma((2, 15)), dma((2,)), dma((2,)),
        ],
        compiler_params=pltpu.CompilerParams(collective_id=0, has_side_effects=True, vmem_limit_bytes=60 << 20),
        name="sums_and_factor",
    )(x, y)


def on_device(first_snaps, next_snaps):
    scale = math.sqrt(first_snaps.shape[0] * lax.axis_size(AXES))
    inverse, cross = sums(first_snaps, next_snaps)
    return finish(inverse, cross, next_snaps, scale)


def solution(mesh):
    finer = Mesh(mesh.devices.reshape(4, 8, 2, 4), AXES)
    spec = P(AXES, None)
    return jax.shard_map(
        on_device, mesh=finer, in_specs=(spec, spec), out_specs=(P(), spec), check_vma=False
    )
```

```python
import functools
import math

import jax
import jax.numpy as jnp
from jax import lax
from jax.experimental import pallas as pl
from jax.experimental.pallas import tpu as pltpu
from jax.sharding import Mesh
from jax.sharding import PartitionSpec as P

AXES = ("y", "z", "c", "x")
MESH = pl.DeviceIdType.MESH
K = 512
NB = 128
F32, BF16 = jnp.float32, jnp.bfloat16
T0 = (((0,), (0,)), ((), ()))
NN = (((1,), (0,)), ((), ()))
NT = (((1,), (1,)), ((), ()))
GROUPS = (
    [(0, j) for j in range(4)],
    [(i, j) for i in range(1, 4) for j in range(i, 4)],
    [(i, j) for i in range(4) for j in range(4)],
)
HALF = [len(blocks) * NB // 2 for blocks in GROUPS]
PIECE = [rows // 16 for rows in HALF]


def split2(x):
    hi = x.astype(BF16)
    return hi, (x - hi.astype(F32)).astype(BF16)


def split3(x):
    hi = x.astype(BF16)
    rest = x - hi.astype(F32)
    mid = rest.astype(BF16)
    return hi, mid, (rest - mid.astype(F32)).astype(BF16)


def mm(a, b, dims):
    return lax.dot_general(a, b, dims, preferred_element_type=F32)


def lane_splat(v, lane):
    return jnp.broadcast_to(v[:, lane : lane + 1], v.shape)


def row_splat(v, row):
    return jnp.broadcast_to(v[row : row + 1, :], v.shape)


def eliminate_block(w, out, midway):
    sub = lax.broadcasted_iota(jnp.int32, (8, NB), 0)
    for t in range(NB // 8):
        if t == 8:
            midway()
        r0 = 8 * t
        pa, pb = w[r0 : r0 + 8, :NB], w[r0 : r0 + 8, NB:]
        s = [lane_splat(pa, r0 + j) for j in range(8)]
        rs, uas, ubs, ums = [], [], [], []
        for j in range(8):
            r = lax.rsqrt(row_splat(s[j], j))
            low = jnp.where(sub > j, s[j] * r, 0.0)
            ua, ub = row_splat(pa, j) * r, row_splat(pb, j) * r
            um = {m: row_splat(s[m], j) * r for m in range(j + 1, 8)}
            for m in um:
                s[m] = s[m] - low * um[m]
            pa, pb = pa - low * ua, pb - low * ub
            out[r0 + j : r0 + j + 1, :] = ub[0:1, :]
            rs.append(r), uas.append(ua), ubs.append(ub), ums.append(um)
        for g in range(t + 1, NB // 8):
            rows = slice(8 * g, 8 * g + 8)
            wa, wb = w[rows, :NB], w[rows, NB:]
            sg = [lane_splat(wa, r0 + j) for j in range(8)]
            for j in range(8):
                low = sg[j] * rs[j]
                for m in range(j + 1, 8):
                    sg[m] = sg[m] - low * ums[j][m]
                wa, wb = wa - low * uas[j], wb - low * ubs[j]
            w[rows, :NB], w[rows, NB:] = wa, wb


def dot6(a3, b3, dims):
    ca, cb = dims[0][0][0], dims[0][1][0]
    ah, am, al = a3
    bh, bm, bl = b3
    left = jnp.concatenate([ah, ah, am, ah, al, am], axis=ca)
    right = jnp.concatenate([bh, bm, bh, bl, bh, bm], axis=cb)
    return mm(left, right, dims)


def invert_factor(z, w, m11, m, midway, after):
    eye = jnp.where(
        lax.broadcasted_iota(jnp.int32, (NB, NB), 0) == lax.broadcasted_iota(jnp.int32, (NB, NB), 1), 1.0, 0.0
    ).astype(F32)
    cols = lax.broadcasted_iota(jnp.int32, (NB, K), 1)
    wide = lax.broadcasted_iota(jnp.int32, (K, K), 1)

    def block_step(kb, carry):
        c0 = pl.multiple_of(kb * NB, NB)
        c1 = c0 + NB
        rows = pl.ds(c0, NB)
        w[:, :NB] = z[rows, rows]
        w[:, NB:] = eye
        eliminate_block(w, m11, lambda: midway(kb))
        z[rows, rows] = eye
        t = dot6(split3(m11[...]), split3(z[rows, :]), NN)
        m[rows, :] = jnp.where(cols < c1, t, 0.0)
        after(kb)

        @pl.when(kb < K // NB - 1)
        def _():
            update = dot6(split3(jnp.where(cols >= c1, t, 0.0)), split3(t), T0)
            z[...] = jnp.where((wide >= c0) & (wide < c1), 0.0, z[...]) - update

        return carry

    lax.fori_loop(0, K // NB, block_step, 0)


def finish_kernel(scale, m_ref, c_ref, modes_ref, red_ref, out_ref, z, sem):
    copy = pltpu.make_async_copy(modes_ref, out_ref, sem)
    copy.start()
    unpack(z, c_ref, 2)
    hi, lo = split2(m_ref[...])
    ch, cl = split2(z[...])
    lh, ll = split2(mm(hi, ch, NN) + mm(hi, cl, NN) + mm(lo, ch, NN))
    red_ref[...] = (mm(lh, hi, NT) + mm(lh, lo, NT) + mm(ll, hi, NT)) * scale
    copy.wait()


def finish(m, cross, modes, scale):
    in_vmem = pl.BlockSpec(memory_space=pltpu.VMEM)
    anywhere = pl.BlockSpec(memory_space=pl.ANY)
    return pl.pallas_call(
        functools.partial(finish_kernel, scale),
        out_shape=(jax.ShapeDtypeStruct((K, K), F32), jax.ShapeDtypeStruct(modes.shape, F32)),
        in_specs=[in_vmem, in_vmem, anywhere],
        out_specs=(in_vmem, anywhere),
        scratch_shapes=[pltpu.VMEM((K, K), F32), pltpu.SemaphoreType.DMA(())],
        compiler_params=pltpu.CompilerParams(vmem_limit_bytes=24 << 20),
        name="operator",
    )(m, cross, modes)


def place(ref, group, i, first, value):
    per = ref.shape[1] // NB
    for n in range(value.shape[1] // NB):
        b = GROUPS[group].index((i, first + n))
        ref[b // per, (b % per) * NB : (b % per + 1) * NB, :] = value[:, n * NB : (n + 1) * NB]


def unpack(z, ref, group):
    per = ref.shape[1] // NB
    for b, (i, j) in enumerate(GROUPS[group]):
        z[i * NB : (i + 1) * NB, j * NB : (j + 1) * NB] = ref[b // per, (b % per) * NB : (b % per + 1) * NB, :]


def sums_kernel(scale, x_hbm, y_hbm, m_out, c_out, mode_out, mh, ml, z, w, m11, xv, yv, xh, xl, yh, yl, g0_out, g1_out,
                loc0, loc1, loc2, other0, other1, other2, chip0, chip1, chip2, land0, land1, cland1, cland2, cpart, cown, mine0, mine1,
                lz0, lz1, lz2, in_sem, d_send, d_recv, xy_send, xy_recv, z_send, z_recv, ag_send, ag_recv, e_send, e_recv,
                c_send, c_recv, f_send, f_recv):
    my, mz, mc, mx = [lax.axis_index(a) for a in AXES]
    oc = 1 - mc
    me = my * 4 + mx
    chunks = xv.shape[0] // 256
    loc, other, chip, land = (loc0, loc1, loc2), (other0, other1, other2), (chip0, chip1, chip2), (land0, land1)
    out = (g0_out, g1_out)
    plane = [(dy, dx) for dy in range(4) for dx in range(4)][1:]

    loads = []
    for n, (src, dst) in enumerate(((x_hbm, xv), (y_hbm, yv))):
        for i in range(chunks):
            part = pl.ds(i * 256, 256)
            loads.append(pltpu.make_async_copy(src.at[part], dst.at[part], in_sem.at[n * chunks + i]))
    for load in loads:
        load.start()

    def in_plane(dy, dx):
        return lax.rem(my + dy + 4, 4), lax.rem(mx + dx + 4, 4)

    def along_z(dz):
        return lax.rem(mz + dz, 8)

    barrier = pltpu.get_barrier_semaphore()
    pl.semaphore_signal(barrier, inc=1, device_id=(my, mz, oc, mx), device_id_type=MESH)
    for dy, dx in plane:
        py, px = in_plane(dy, dx)
        pl.semaphore_signal(barrier, inc=1, device_id=(py, mz, mc, px), device_id_type=MESH)
    for dz in range(1, 8):
        pl.semaphore_signal(barrier, inc=1, device_id=(my, along_z(dz), mc, mx), device_id_type=MESH)

    def piece(ref, who, size):
        return ref.at[pl.ds(pl.multiple_of(who * size, 8), size), :]

    def to_partner(src, dst, sends, recvs):
        return pltpu.make_async_remote_copy(src, dst, sends, recvs, device_id=(my, mz, oc, mx), device_id_type=MESH)

    def to_plane(src, dst, k, sends, recvs):
        py, px = in_plane(*plane[k])
        return pltpu.make_async_remote_copy(src, dst, sends, recvs, device_id=(py, mz, mc, px), device_id_type=MESH)

    def to_z(src, dst, k, sends, recvs):
        return pltpu.make_async_remote_copy(src, dst, sends, recvs, device_id=(my, along_z(k + 1), mc, mx), device_id_type=MESH)

    def start(copies):
        for c in copies:
            c.start()
        return copies

    def wait(copies):
        for c in copies:
            c.wait()

    def pair(n):
        return start([to_partner(loc[n].at[oc], other[n], d_send.at[n], d_recv.at[n])])

    def scatter(n, copies):
        wait(copies)
        chip[n][...] = loc[n][mc] + other[n][...]
        made = []
        for k in range(15):
            py, px = in_plane(*plane[k])
            made.append(to_plane(piece(chip[n], py * 4 + px, PIECE[n]), land[n].at[k], k, xy_send.at[n, k], xy_recv.at[n, k]))
        return start(made)

    def plane_sum(n, copies):
        wait(copies)
        total = chip[n][pl.ds(pl.multiple_of(me * PIECE[n], 8), PIECE[n]), :]
        for k in range(15):
            total = total + land[n][k]
        return total

    def spread_z(n, copies):
        mine, lz = ((mine0, lz0), (mine1, lz1))[n]
        total = plane_sum(n, copies)
        mine[...] = total
        lz[mz] = total
        return start([to_z(mine, lz.at[mz], k, z_send.at[n, k], z_recv.at[n, k]) for k in range(7)])

    def gather_plane(n):
        mine = piece(out[n].at[mc], me, PIECE[n])
        made = start([to_plane(mine, mine, k, ag_send.at[n, k], ag_recv.at[n, k]) for k in range(15)])
        return made, start([to_partner(mine, mine, e_send.at[n, 15], e_recv.at[n, 15])])

    def gather(n, copies):
        lz = (lz0, lz1)[n]
        wait(copies)
        total = lz[0]
        for k in range(1, 8):
            total = total + lz[k]
        out[n][mc, pl.ds(pl.multiple_of(me * PIECE[n], 8), PIECE[n]), :] = total
        return gather_plane(n)

    def pass_on(n, state):
        made, sent = state
        for k, (dy, dx) in enumerate(plane):
            made[k].wait_recv()
            py, px = in_plane(-dy, -dx)
            landed = piece(out[n].at[mc], py * 4 + px, PIECE[n])
            sent = sent + start([to_partner(landed, landed, e_send.at[n, k], e_recv.at[n, k])])
        for c in made:
            c.wait_send()
        return sent

    a_rows = lambda x, y: x * NB + y * 32
    b_rows = lambda y, x: HALF[2] // 2 + y * NB + x * 32

    def line(half, along_x, d):
        return (my, mz, mc, lax.rem(mx + d + 4, 4)) if along_x else (lax.rem(my + d + 4, 4), mz, mc, mx)

    def on_line(stage, half, along_x, d, src, dst):
        return pltpu.make_async_remote_copy(src, dst, c_send.at[stage, half, d - 1], c_recv.at[stage, half, d - 1],
                                            device_id=line(half, along_x, d), device_id_type=MESH)

    def aligned(ref, first, size):
        return ref.at[pl.ds(pl.multiple_of(first, 8), size), :]

    def cross_first(copies):
        wait(copies)
        chip2[...] = loc2[mc] + other2[...]
        made = []
        for d in (1, 2, 3):
            made.append(on_line(0, 0, True, d, aligned(chip2, a_rows(lax.rem(mx + d, 4), 0), NB), cland1.at[0, d - 1]))
            made.append(on_line(0, 1, False, d, aligned(chip2, b_rows(lax.rem(my + d, 4), 0), NB), cland1.at[1, d - 1]))
        return start(made)

    def cross_second(copies):
        wait(copies)
        for half, first in ((0, a_rows(mx, 0)), (1, b_rows(my, 0))):
            cpart[half] = chip2[pl.ds(pl.multiple_of(first, 8), NB), :] + cland1[half, 0] + cland1[half, 1] + cland1[half, 2]
        made = []
        for d in (1, 2, 3):
            made.append(on_line(1, 0, False, d, aligned(cpart.at[0], lax.rem(my + d, 4) * 32, 32), cland2.at[0, d - 1]))
            made.append(on_line(1, 1, True, d, aligned(cpart.at[1], lax.rem(mx + d, 4) * 32, 32), cland2.at[1, d - 1]))
        return start(made)

    def cross_z(copies):
        wait(copies)
        for half, first in ((0, my * 32), (1, mx * 32)):
            cown[half * 32 : half * 32 + 32, :] = (
                cpart[half, pl.ds(pl.multiple_of(first, 8), 32), :] + cland2[half, 0] + cland2[half, 1] + cland2[half, 2]
            )

    upper = mz // 4
    own = pl.ds(pl.multiple_of((1 - upper) * a_rows(mx, my) + upper * b_rows(my, mx) + lax.rem(mz, 4) * 8, 8), 8)

    def cross_back(copies):
        wait(copies)
        total = cown[pl.ds(pl.multiple_of(mz * 8, 8), 8), :]
        for k in range(7):
            total = total + lz2[k]
        c_out[mc, own, :] = total

    def cross_lines(stage, size, swap):
        made = []
        for d in (1, 2, 3):
            for half, first in ((0, a_rows(mx, 0 if swap else my)), (1, b_rows(my, 0 if swap else mx))):
                rows = aligned(c_out.at[mc], first, size)
                made.append(on_line(stage, half, (half == 0) == swap, d, rows, rows))
        return made

    def cross_forwards():
        made = [(0, a_rows(mx, 0)), (4, b_rows(my, 0))]
        for d in (1, 2, 3):
            made += [(d, a_rows(lax.rem(mx - d + 4, 4), 0)), (4 + d, b_rows(lax.rem(my - d + 4, 4), 0))]
        return [to_partner(aligned(c_out.at[mc], first, NB), aligned(c_out.at[mc], first, NB), f_send.at[k], f_recv.at[k])
                for k, first in made]

    for i in range(chunks):
        loads[i].wait()
        part = slice(i * 256, i * 256 + 256)
        xh[part, :], xl[part, :] = split2(xv[part, :])

    def gram_band(c0, c1):
        h, l, h2, l2 = xh[:, c0:c1], xl[:, c0:c1], xh[:, c0:], xl[:, c0:]
        return mm(h, h2, T0) + mm(h, l2, T0) + mm(l, h2, T0) + mm(l, l2, T0)

    place(loc0, 0, 0, 0, gram_band(0, NB))
    pl.semaphore_wait(barrier, 1 + len(plane) + 7)
    g0 = pair(0)
    place(loc1, 1, 1, 1, gram_band(NB, 2 * NB))
    g = gram_band(2 * NB, K)
    place(loc1, 1, 2, 2, g[:NB])
    place(loc1, 1, 3, 3, g[NB:, NB:])
    g1 = pair(1)
    g0 = scatter(0, g0)
    for i in range(chunks):
        loads[chunks + i].wait()
        part = slice(i * 256, i * 256 + 256)
        yh[part, :], yl[part, :] = split2(yv[part, :])
    g1 = scatter(1, g1)
    def cross_bands(bands):
        for i in bands:
            h, l = xh[:, i * NB : (i + 1) * NB], xl[:, i * NB : (i + 1) * NB]
            place(loc2, 2, i, 0, mm(h, yh[...], T0) + mm(h, yl[...], T0) + mm(l, yh[...], T0))

    cross_bands((0, 1))
    g0 = spread_z(0, g0)
    cross_bands((2, 3))
    c = pair(2)
    g1 = spread_z(1, g1)
    c = cross_first(c)
    g0 = gather(0, g0)
    g1 = gather(1, g1)
    c = cross_second(c)
    g0 = pass_on(0, g0)
    c_over = [to_z(piece(cown, along_z(k + 1), 8), lz2.at[k], k, z_send.at[2, k], z_recv.at[2, k]) for k in range(7)]
    c_rows = c_out.at[mc, own, :]
    c_back = [to_z(c_rows, c_rows, k, z_send.at[3, k], z_recv.at[3, k]) for k in range(7)]
    c_third = cross_lines(2, 32, False)
    c_fourth = cross_lines(3, NB, True)
    c_sent = cross_forwards()

    def awaited(n):
        copies = []
        for k, (dy, dx) in enumerate(plane):
            py, px = in_plane(-dy, -dx)
            landed = piece(out[n].at[mc], py * 4 + px, PIECE[n])
            copies.append(to_partner(landed, landed, e_send.at[n, k], e_recv.at[n, k]))
        mine = piece(out[n].at[mc], me, PIECE[n])
        return copies + [to_partner(mine, mine, e_send.at[n, 15], e_recv.at[n, 15])]

    def midway(kb):
        @pl.when(kb == 0)
        def _():
            pass_on(1, g1)
            cross_z(c)
            start(c_over)

        @pl.when(kb == 1)
        def _():
            cross_back(c_over)
            start(c_back)

        @pl.when(kb == 2)
        def _():
            wait(c_back)
            start(c_third)

    def after(kb):
        @pl.when(kb == 0)
        def _():
            wait(awaited(1))
            unpack(z, g1_out, 1)

        @pl.when(kb == 2)
        def _():
            wait(c_third)
            start(c_fourth)
            start(c_sent[:2])

    wait(g0)
    unpack(z, g0_out, 0)
    invert_factor(z, w, m11, m_out, midway, after)

    mh[...], ml[...] = split2(m_out[...])

    def modes(i, carry):
        rows = pl.ds(pl.multiple_of(i * 256, 256), 256)
        for n, k1 in ((0, 256), (256, 512)):
            ph, plo = mh[n : n + 256, :k1], ml[n : n + 256, :k1]
            ah, al = yh[rows, :k1], yl[rows, :k1]
            mode_out[rows, n : n + 256] = (mm(ah, ph, NT) + mm(ah, plo, NT) + mm(al, ph, NT)) * scale
        @pl.when(i == 1)
        def _():
            for k, copy in enumerate(c_fourth):
                copy.wait_recv()
                c_sent[2 + k].start()
            for copy in c_fourth:
                copy.wait_send()

        return carry

    lax.fori_loop(0, chunks, modes, 0)
    wait(c_sent)


def sums(x, y, scale):
    rows = x.shape[0]
    vm = pltpu.VMEM
    dma = pltpu.SemaphoreType.DMA
    per_group = lambda lead, sizes: [vm((*lead, size, NB), F32) for size in sizes]
    return pl.pallas_call(
        functools.partial(sums_kernel, scale),
        out_shape=(
            jax.ShapeDtypeStruct((K, K), F32),
            jax.ShapeDtypeStruct((2, HALF[2], NB), F32),
            jax.ShapeDtypeStruct((rows, K), F32),
        ),
        in_specs=[pl.BlockSpec(memory_space=pltpu.MemorySpace.HBM)] * 2,
        out_specs=(pl.BlockSpec(memory_space=pltpu.VMEM),) * 3,
        scratch_shapes=[
            vm((K, K), BF16), vm((K, K), BF16),
            vm((K, K), F32), vm((NB, 2 * NB), F32), vm((NB, NB), F32),
            vm((rows, K), F32), vm((rows, K), F32),
            vm((rows, K), BF16), vm((rows, K), BF16), vm((rows, K), BF16), vm((rows, K), BF16),
            *per_group((2,), HALF[:2]),
            *per_group((2,), HALF), *per_group((), HALF), *per_group((), HALF), *per_group((15,), PIECE[:2]),
            vm((2, 3, NB, NB), F32), vm((2, 3, 32, NB), F32), vm((2, NB, NB), F32), vm((64, NB), F32),
            *per_group((), PIECE[:2]), *per_group((8,), PIECE[:2]), vm((7, 8, NB), F32),
            dma((2 * (rows // 256),)), dma((3,)), dma((3,)), dma((2, 15)), dma((2, 15)), dma((4, 7)), dma((4, 7)),
            dma((2, 15)), dma((2, 15)), dma((2, 16)), dma((2, 16)), dma((4, 2, 3)), dma((4, 2, 3)), dma((8,)), dma((8,)),
        ],
        compiler_params=pltpu.CompilerParams(collective_id=0, has_side_effects=True, vmem_limit_bytes=32 << 20),
        name="sums_and_factor",
    )(x, y)


def on_device(first_snaps, next_snaps):
    scale = math.sqrt(first_snaps.shape[0] * lax.axis_size(AXES))
    hbm = pltpu.MemorySpace.HBM
    in_hbm = [pltpu.with_memory_space_constraint(a, hbm) for a in (first_snaps, next_snaps)]
    inverse, cross, modes = sums(*in_hbm, scale)
    return finish(inverse, cross, modes, scale)


def solution(mesh):
    finer = Mesh(mesh.devices.reshape(4, 8, 2, 4), AXES)
    spec = P(AXES, None)
    return jax.shard_map(
        on_device, mesh=finer, in_specs=(spec, spec), out_specs=(P(), spec), check_vma=False
    )
```

```python
import functools
import math

import jax
import jax.numpy as jnp
from jax import lax
from jax.experimental import pallas as pl
from jax.experimental.pallas import tpu as pltpu
from jax.sharding import Mesh
from jax.sharding import PartitionSpec as P

AXES = ("y", "z", "c", "x")
MESH = pl.DeviceIdType.MESH
K = 512
NB = 128
F32, BF16 = jnp.float32, jnp.bfloat16
T0 = (((0,), (0,)), ((), ()))
NN = (((1,), (0,)), ((), ()))
NT = (((1,), (1,)), ((), ()))
GROUPS = (
    [(0, j) for j in range(4)],
    [(i, j) for i in range(1, 4) for j in range(i, 4)],
    [(i, j) for i in range(4) for j in range(4)],
)
HALF = [len(blocks) * NB // 2 for blocks in GROUPS]
PIECE = [rows // 16 for rows in HALF]


def split2(x):
    hi = x.astype(BF16)
    return hi, (x - hi.astype(F32)).astype(BF16)


def split3(x):
    hi = x.astype(BF16)
    rest = x - hi.astype(F32)
    mid = rest.astype(BF16)
    return hi, mid, (rest - mid.astype(F32)).astype(BF16)


def mm(a, b, dims):
    return lax.dot_general(a, b, dims, preferred_element_type=F32)


def lane_splat(v, lane):
    return jnp.broadcast_to(v[:, lane : lane + 1], v.shape)


def row_splat(v, row):
    return jnp.broadcast_to(v[row : row + 1, :], v.shape)


def eliminate_block(w, out, midway):
    sub = lax.broadcasted_iota(jnp.int32, (8, NB), 0)
    lane = lax.broadcasted_iota(jnp.int32, (8, NB), 1)
    p = w[0:8, :]
    s = [lane_splat(p, j) for j in range(8)]
    for t in range(NB // 8):
        if t == 8:
            midway()
        r0 = 8 * t
        more = t + 1 < NB // 8
        inside = (lane >= r0) & (lane < r0 + 8)
        p = jnp.where(inside, jnp.where(sub == lane - r0, 1.0, 0.0), p)
        if more:
            na = w[r0 + 8 : r0 + 16, :]
            nn = [lane_splat(na, r0 + j) for j in range(8)]
            nx = [lane_splat(na, r0 + 8 + m) for m in range(8)]
            na = jnp.where(inside, 0.0, na)
        rs, us, ums, done = [], [], [], p
        for j in range(8):
            r = lax.rsqrt(row_splat(s[j], j))
            low = jnp.where(sub > j, s[j] * r, 0.0)
            um = {m: row_splat(s[m], j) * r for m in range(j + 1, 8)}
            for m in um:
                s[m] = s[m] - low * um[m]
            u = row_splat(p, j) * r
            p = p - low * u
            done = jnp.where(sub == j, u, done)
            if more:
                ln = nn[j] * r
                for m in um:
                    nn[m] = nn[m] - ln * um[m]
                na = na - ln * u
                for m in range(8):
                    nx[m] = nx[m] - ln * row_splat(ln, m)
            rs.append(r), us.append(u), ums.append(um)
        out[r0 : r0 + 8, :] = jnp.where(lane < r0 + 8, done, 0.0)
        for g in range(t + 2, NB // 8):
            rows = slice(8 * g, 8 * g + 8)
            wa = w[rows, :]
            sg = [lane_splat(wa, r0 + j) for j in range(8)]
            wa = jnp.where(inside, 0.0, wa)
            for j in range(8):
                low = sg[j] * rs[j]
                for m in range(j + 1, 8):
                    sg[m] = sg[m] - low * ums[j][m]
                wa = wa - low * us[j]
            w[rows, :] = wa
        if more:
            p, s = na, nx


def dot6(a3, b3, dims):
    ca, cb = dims[0][0][0], dims[0][1][0]
    ah, am, al = a3
    bh, bm, bl = b3
    left = jnp.concatenate([ah, ah, am, ah, al, am], axis=ca)
    right = jnp.concatenate([bh, bm, bh, bl, bh, bm], axis=cb)
    return mm(left, right, dims)


def invert_factor(z, w, m11, m, midway, after):
    eye = jnp.where(
        lax.broadcasted_iota(jnp.int32, (NB, NB), 0) == lax.broadcasted_iota(jnp.int32, (NB, NB), 1), 1.0, 0.0
    ).astype(F32)
    cols = lax.broadcasted_iota(jnp.int32, (NB, K), 1)
    wide = lax.broadcasted_iota(jnp.int32, (K, K), 1)

    def block_step(kb, carry):
        c0 = pl.multiple_of(kb * NB, NB)
        c1 = c0 + NB
        rows = pl.ds(c0, NB)
        w[...] = z[rows, rows]
        eliminate_block(w, m11, lambda: midway(kb))
        z[rows, rows] = eye
        t = dot6(split3(m11[...]), split3(z[rows, :]), NN)
        m[rows, :] = jnp.where(cols < c1, t, 0.0)
        after(kb)

        @pl.when(kb < K // NB - 1)
        def _():
            update = dot6(split3(jnp.where(cols >= c1, t, 0.0)), split3(t), T0)
            z[...] = jnp.where((wide >= c0) & (wide < c1), 0.0, z[...]) - update

        return carry

    lax.fori_loop(0, K // NB, block_step, 0)


def finish_kernel(scale, m_ref, c_ref, modes_ref, red_ref, out_ref, z, sem):
    copy = pltpu.make_async_copy(modes_ref, out_ref, sem)
    copy.start()
    unpack(z, c_ref, 2)
    hi, lo = split2(m_ref[...])
    ch, cl = split2(z[...])
    lh, ll = split2(mm(hi, ch, NN) + mm(hi, cl, NN) + mm(lo, ch, NN))
    red_ref[...] = (mm(lh, hi, NT) + mm(lh, lo, NT) + mm(ll, hi, NT)) * scale
    copy.wait()


def finish(m, cross, modes, scale):
    in_vmem = pl.BlockSpec(memory_space=pltpu.VMEM)
    anywhere = pl.BlockSpec(memory_space=pl.ANY)
    return pl.pallas_call(
        functools.partial(finish_kernel, scale),
        out_shape=(jax.ShapeDtypeStruct((K, K), F32), jax.ShapeDtypeStruct(modes.shape, F32)),
        in_specs=[in_vmem, in_vmem, anywhere],
        out_specs=(in_vmem, anywhere),
        scratch_shapes=[pltpu.VMEM((K, K), F32), pltpu.SemaphoreType.DMA(())],
        compiler_params=pltpu.CompilerParams(vmem_limit_bytes=24 << 20),
        name="operator",
    )(m, cross, modes)


def place(ref, group, i, first, value):
    per = ref.shape[1] // NB
    for n in range(value.shape[1] // NB):
        b = GROUPS[group].index((i, first + n))
        ref[b // per, (b % per) * NB : (b % per + 1) * NB, :] = value[:, n * NB : (n + 1) * NB]


def unpack(z, ref, group):
    per = ref.shape[1] // NB
    for b, (i, j) in enumerate(GROUPS[group]):
        z[i * NB : (i + 1) * NB, j * NB : (j + 1) * NB] = ref[b // per, (b % per) * NB : (b % per + 1) * NB, :]


def sums_kernel(scale, x_hbm, y_hbm, m_out, c_out, mode_out, mh, ml, z, w, m11, xv, yv, xh, xl, yh, yl, g0_out, g1_out,
                loc0, loc1, loc2, other0, other1, other2, chip0, chip1, chip2, land0, land1, cland1, cland2, cpart, cown, mine0, mine1,
                lz0, lz1, lz2, in_sem, d_send, d_recv, xy_send, xy_recv, z_send, z_recv, ag_send, ag_recv, e_send, e_recv,
                c_send, c_recv, f_send, f_recv):
    my, mz, mc, mx = [lax.axis_index(a) for a in AXES]
    oc = 1 - mc
    me = my * 4 + mx
    chunks = xv.shape[0] // 256
    loc, other, chip, land = (loc0, loc1, loc2), (other0, other1, other2), (chip0, chip1, chip2), (land0, land1)
    out = (g0_out, g1_out)
    plane = [(dy, dx) for dy in range(4) for dx in range(4)][1:]

    loads = []
    for n, (src, dst) in enumerate(((x_hbm, xv), (y_hbm, yv))):
        for i in range(chunks):
            part = pl.ds(i * 256, 256)
            loads.append(pltpu.make_async_copy(src.at[part], dst.at[part], in_sem.at[n * chunks + i]))
    for load in loads:
        load.start()

    def in_plane(dy, dx):
        return lax.rem(my + dy + 4, 4), lax.rem(mx + dx + 4, 4)

    def along_z(dz):
        return lax.rem(mz + dz, 8)

    barrier = pltpu.get_barrier_semaphore()
    pl.semaphore_signal(barrier, inc=1, device_id=(my, mz, oc, mx), device_id_type=MESH)
    for dy, dx in plane:
        py, px = in_plane(dy, dx)
        pl.semaphore_signal(barrier, inc=1, device_id=(py, mz, mc, px), device_id_type=MESH)
    for dz in range(1, 8):
        pl.semaphore_signal(barrier, inc=1, device_id=(my, along_z(dz), mc, mx), device_id_type=MESH)

    def piece(ref, who, size):
        return ref.at[pl.ds(pl.multiple_of(who * size, 8), size), :]

    def to_partner(src, dst, sends, recvs):
        return pltpu.make_async_remote_copy(src, dst, sends, recvs, device_id=(my, mz, oc, mx), device_id_type=MESH)

    def to_plane(src, dst, k, sends, recvs):
        py, px = in_plane(*plane[k])
        return pltpu.make_async_remote_copy(src, dst, sends, recvs, device_id=(py, mz, mc, px), device_id_type=MESH)

    def to_z(src, dst, k, sends, recvs):
        return pltpu.make_async_remote_copy(src, dst, sends, recvs, device_id=(my, along_z(k + 1), mc, mx), device_id_type=MESH)

    def start(copies):
        for c in copies:
            c.start()
        return copies

    def wait(copies):
        for c in copies:
            c.wait()

    def pair(n):
        return start([to_partner(loc[n].at[oc], other[n], d_send.at[n], d_recv.at[n])])

    def scatter(n, copies):
        wait(copies)
        chip[n][...] = loc[n][mc] + other[n][...]
        made = []
        for k in range(15):
            py, px = in_plane(*plane[k])
            made.append(to_plane(piece(chip[n], py * 4 + px, PIECE[n]), land[n].at[k], k, xy_send.at[n, k], xy_recv.at[n, k]))
        return start(made)

    def plane_sum(n, copies):
        wait(copies)
        total = chip[n][pl.ds(pl.multiple_of(me * PIECE[n], 8), PIECE[n]), :]
        for k in range(15):
            total = total + land[n][k]
        return total

    def spread_z(n, copies):
        mine, lz = ((mine0, lz0), (mine1, lz1))[n]
        total = plane_sum(n, copies)
        mine[...] = total
        lz[mz] = total
        return start([to_z(mine, lz.at[mz], k, z_send.at[n, k], z_recv.at[n, k]) for k in range(7)])

    def gather_plane(n):
        mine = piece(out[n].at[mc], me, PIECE[n])
        made = start([to_plane(mine, mine, k, ag_send.at[n, k], ag_recv.at[n, k]) for k in range(15)])
        return made, start([to_partner(mine, mine, e_send.at[n, 15], e_recv.at[n, 15])])

    def gather(n, copies):
        lz = (lz0, lz1)[n]
        wait(copies)
        total = lz[0]
        for k in range(1, 8):
            total = total + lz[k]
        out[n][mc, pl.ds(pl.multiple_of(me * PIECE[n], 8), PIECE[n]), :] = total
        return gather_plane(n)

    def pass_on(n, state):
        made, sent = state
        for k, (dy, dx) in enumerate(plane):
            made[k].wait_recv()
            py, px = in_plane(-dy, -dx)
            landed = piece(out[n].at[mc], py * 4 + px, PIECE[n])
            sent = sent + start([to_partner(landed, landed, e_send.at[n, k], e_recv.at[n, k])])
        for c in made:
            c.wait_send()
        return sent

    a_rows = lambda x, y: x * NB + y * 32
    b_rows = lambda y, x: HALF[2] // 2 + y * NB + x * 32

    def line(half, along_x, d):
        return (my, mz, mc, lax.rem(mx + d + 4, 4)) if along_x else (lax.rem(my + d + 4, 4), mz, mc, mx)

    def on_line(stage, half, along_x, d, src, dst):
        return pltpu.make_async_remote_copy(src, dst, c_send.at[stage, half, d - 1], c_recv.at[stage, half, d - 1],
                                            device_id=line(half, along_x, d), device_id_type=MESH)

    def aligned(ref, first, size):
        return ref.at[pl.ds(pl.multiple_of(first, 8), size), :]

    def cross_first(copies):
        wait(copies)
        chip2[...] = loc2[mc] + other2[...]
        made = []
        for d in (1, 2, 3):
            made.append(on_line(0, 0, True, d, aligned(chip2, a_rows(lax.rem(mx + d, 4), 0), NB), cland1.at[0, d - 1]))
            made.append(on_line(0, 1, False, d, aligned(chip2, b_rows(lax.rem(my + d, 4), 0), NB), cland1.at[1, d - 1]))
        return start(made)

    def cross_second(copies):
        wait(copies)
        for half, first in ((0, a_rows(mx, 0)), (1, b_rows(my, 0))):
            cpart[half] = chip2[pl.ds(pl.multiple_of(first, 8), NB), :] + cland1[half, 0] + cland1[half, 1] + cland1[half, 2]
        made = []
        for d in (1, 2, 3):
            made.append(on_line(1, 0, False, d, aligned(cpart.at[0], lax.rem(my + d, 4) * 32, 32), cland2.at[0, d - 1]))
            made.append(on_line(1, 1, True, d, aligned(cpart.at[1], lax.rem(mx + d, 4) * 32, 32), cland2.at[1, d - 1]))
        return start(made)

    def cross_z(copies):
        wait(copies)
        for half, first in ((0, my * 32), (1, mx * 32)):
            cown[half * 32 : half * 32 + 32, :] = (
                cpart[half, pl.ds(pl.multiple_of(first, 8), 32), :] + cland2[half, 0] + cland2[half, 1] + cland2[half, 2]
            )

    upper = mz // 4
    own = pl.ds(pl.multiple_of((1 - upper) * a_rows(mx, my) + upper * b_rows(my, mx) + lax.rem(mz, 4) * 8, 8), 8)

    def cross_back(copies):
        wait(copies)
        total = cown[pl.ds(pl.multiple_of(mz * 8, 8), 8), :]
        for k in range(7):
            total = total + lz2[k]
        c_out[mc, own, :] = total

    def cross_lines(stage, size, swap):
        made = []
        for d in (1, 2, 3):
            for half, first in ((0, a_rows(mx, 0 if swap else my)), (1, b_rows(my, 0 if swap else mx))):
                rows = aligned(c_out.at[mc], first, size)
                made.append(on_line(stage, half, (half == 0) == swap, d, rows, rows))
        return made

    def cross_forwards():
        made = [(0, a_rows(mx, 0)), (4, b_rows(my, 0))]
        for d in (1, 2, 3):
            made += [(d, a_rows(lax.rem(mx - d + 4, 4), 0)), (4 + d, b_rows(lax.rem(my - d + 4, 4), 0))]
        return [to_partner(aligned(c_out.at[mc], first, NB), aligned(c_out.at[mc], first, NB), f_send.at[k], f_recv.at[k])
                for k, first in made]

    for i in range(chunks):
        loads[i].wait()
        part = slice(i * 256, i * 256 + 256)
        xh[part, :], xl[part, :] = split2(xv[part, :])

    def gram_band(c0, c1):
        h, l, h2, l2 = xh[:, c0:c1], xl[:, c0:c1], xh[:, c0:], xl[:, c0:]
        return mm(h, h2, T0) + mm(h, l2, T0) + mm(l, h2, T0) + mm(l, l2, T0)

    place(loc0, 0, 0, 0, gram_band(0, NB))
    pl.semaphore_wait(barrier, 1 + len(plane) + 7)
    g0 = pair(0)
    place(loc1, 1, 1, 1, gram_band(NB, 2 * NB))
    g = gram_band(2 * NB, K)
    place(loc1, 1, 2, 2, g[:NB])
    place(loc1, 1, 3, 3, g[NB:, NB:])
    g1 = pair(1)
    g0 = scatter(0, g0)
    for i in range(chunks):
        loads[chunks + i].wait()
        part = slice(i * 256, i * 256 + 256)
        yh[part, :], yl[part, :] = split2(yv[part, :])
    g1 = scatter(1, g1)
    def cross_half(half):
        for i in range(2):
            band = pl.ds(pl.multiple_of((half * 2 + i) * NB, NB), NB)
            h, l = xh[:, band], xl[:, band]
            value = mm(h, yh[...], T0) + mm(h, yl[...], T0) + mm(l, yh[...], T0)
            for j in range(4):
                loc2[half, (4 * i + j) * NB : (4 * i + j + 1) * NB, :] = value[:, j * NB : (j + 1) * NB]

    cross_half(oc)
    c = pair(2)
    g0 = spread_z(0, g0)
    cross_half(mc)
    c = cross_first(c)
    g1 = spread_z(1, g1)
    g0 = gather(0, g0)
    c = cross_second(c)
    g1 = gather(1, g1)
    g0 = pass_on(0, g0)
    c_over = [to_z(piece(cown, along_z(k + 1), 8), lz2.at[k], k, z_send.at[2, k], z_recv.at[2, k]) for k in range(7)]
    c_rows = c_out.at[mc, own, :]
    c_back = [to_z(c_rows, c_rows, k, z_send.at[3, k], z_recv.at[3, k]) for k in range(7)]
    c_third = cross_lines(2, 32, False)
    c_fourth = cross_lines(3, NB, True)
    c_sent = cross_forwards()

    def awaited(n):
        copies = []
        for k, (dy, dx) in enumerate(plane):
            py, px = in_plane(-dy, -dx)
            landed = piece(out[n].at[mc], py * 4 + px, PIECE[n])
            copies.append(to_partner(landed, landed, e_send.at[n, k], e_recv.at[n, k]))
        mine = piece(out[n].at[mc], me, PIECE[n])
        return copies + [to_partner(mine, mine, e_send.at[n, 15], e_recv.at[n, 15])]

    def midway(kb):
        @pl.when(kb == 0)
        def _():
            pass_on(1, g1)

        @pl.when(kb == 2)
        def _():
            wait(c_back)
            start(c_third)

        @pl.when(kb == 3)
        def _():
            wait(c_third)
            start(c_fourth)
            start(c_sent[:2])

    def after(kb):
        @pl.when(kb == 0)
        def _():
            wait(awaited(1))
            unpack(z, g1_out, 1)
            cross_back(c_over)
            start(c_back)

    cross_z(c)
    start(c_over)
    wait(g0)
    unpack(z, g0_out, 0)
    invert_factor(z, w, m11, m_out, midway, after)

    mh[...], ml[...] = split2(m_out[...])

    def modes(i, carry):
        rows = pl.ds(pl.multiple_of(i * 256, 256), 256)
        for n, k1 in ((0, 256), (256, 512)):
            ph, plo = mh[n : n + 256, :k1], ml[n : n + 256, :k1]
            ah, al = yh[rows, :k1], yl[rows, :k1]
            mode_out[rows, n : n + 256] = (mm(ah, ph, NT) + mm(ah, plo, NT) + mm(al, ph, NT)) * scale
        return carry

    lax.fori_loop(0, chunks, modes, 0)
    for k, copy in enumerate(c_fourth):
        copy.wait_recv()
        c_sent[2 + k].start()
    for copy in c_fourth:
        copy.wait_send()
    wait(c_sent)


def sums(x, y, scale):
    rows = x.shape[0]
    vm = pltpu.VMEM
    dma = pltpu.SemaphoreType.DMA
    per_group = lambda lead, sizes: [vm((*lead, size, NB), F32) for size in sizes]
    return pl.pallas_call(
        functools.partial(sums_kernel, scale),
        out_shape=(
            jax.ShapeDtypeStruct((K, K), F32),
            jax.ShapeDtypeStruct((2, HALF[2], NB), F32),
            jax.ShapeDtypeStruct((rows, K), F32),
        ),
        in_specs=[pl.BlockSpec(memory_space=pltpu.MemorySpace.HBM)] * 2,
        out_specs=(pl.BlockSpec(memory_space=pltpu.VMEM),) * 3,
        scratch_shapes=[
            vm((K, K), BF16), vm((K, K), BF16),
            vm((K, K), F32), vm((NB, NB), F32), vm((NB, NB), F32),
            vm((rows, K), F32), vm((rows, K), F32),
            vm((rows, K), BF16), vm((rows, K), BF16), vm((rows, K), BF16), vm((rows, K), BF16),
            *per_group((2,), HALF[:2]),
            *per_group((2,), HALF), *per_group((), HALF), *per_group((), HALF), *per_group((15,), PIECE[:2]),
            vm((2, 3, NB, NB), F32), vm((2, 3, 32, NB), F32), vm((2, NB, NB), F32), vm((64, NB), F32),
            *per_group((), PIECE[:2]), *per_group((8,), PIECE[:2]), vm((7, 8, NB), F32),
            dma((2 * (rows // 256),)), dma((3,)), dma((3,)), dma((2, 15)), dma((2, 15)), dma((4, 7)), dma((4, 7)),
            dma((2, 15)), dma((2, 15)), dma((2, 16)), dma((2, 16)), dma((4, 2, 3)), dma((4, 2, 3)), dma((8,)), dma((8,)),
        ],
        compiler_params=pltpu.CompilerParams(collective_id=0, has_side_effects=True, vmem_limit_bytes=32 << 20),
        name="sums_and_factor",
    )(x, y)


def on_device(first_snaps, next_snaps):
    scale = math.sqrt(first_snaps.shape[0] * lax.axis_size(AXES))
    hbm = pltpu.MemorySpace.HBM
    in_hbm = [pltpu.with_memory_space_constraint(a, hbm) for a in (first_snaps, next_snaps)]
    inverse, cross, modes = sums(*in_hbm, scale)
    return finish(inverse, cross, modes, scale)


def solution(mesh):
    finer = Mesh(mesh.devices.reshape(4, 8, 2, 4), AXES)
    spec = P(AXES, None)
    return jax.shard_map(
        on_device, mesh=finer, in_specs=(spec, spec), out_specs=(P(), spec), check_vma=False
    )
```

```python
import functools
import math

import jax
import jax.numpy as jnp
from jax import lax
from jax.experimental import pallas as pl
from jax.experimental.pallas import tpu as pltpu
from jax.sharding import Mesh
from jax.sharding import PartitionSpec as P

AXES = ("y", "z", "c", "x")
MESH = pl.DeviceIdType.MESH
K = 512
NB = 128
F32, BF16 = jnp.float32, jnp.bfloat16
T0 = (((0,), (0,)), ((), ()))
NN = (((1,), (0,)), ((), ()))
NT = (((1,), (1,)), ((), ()))
GROUPS = (
    [(0, j) for j in range(4)],
    [(i, j) for i in range(1, 4) for j in range(i, 4)],
    [(i, j) for i in range(4) for j in range(4)],
)
HALF = [len(blocks) * NB // 2 for blocks in GROUPS]
PIECE = [rows // 16 for rows in HALF]


def split2(x):
    hi = x.astype(BF16)
    return hi, (x - hi.astype(F32)).astype(BF16)


def split3(x):
    hi = x.astype(BF16)
    rest = x - hi.astype(F32)
    mid = rest.astype(BF16)
    return hi, mid, (rest - mid.astype(F32)).astype(BF16)


def mm(a, b, dims):
    return lax.dot_general(a, b, dims, preferred_element_type=F32)


def lane_splat(v, lane):
    return jnp.broadcast_to(v[:, lane : lane + 1], v.shape)


def row_splat(v, row):
    return jnp.broadcast_to(v[row : row + 1, :], v.shape)


def eliminate_block(w, out, midway):
    sub = lax.broadcasted_iota(jnp.int32, (8, NB), 0)
    lane = lax.broadcasted_iota(jnp.int32, (8, NB), 1)
    p = w[0:8, :]
    s = [lane_splat(p, j) for j in range(8)]
    for t in range(NB // 8):
        if t == 8:
            midway()
        r0 = 8 * t
        more = t + 1 < NB // 8
        inside = (lane >= r0) & (lane < r0 + 8)
        p = jnp.where(inside, jnp.where(sub == lane - r0, 1.0, 0.0), p)
        if more:
            na = w[r0 + 8 : r0 + 16, :]
            nn = [lane_splat(na, r0 + j) for j in range(8)]
            nx = [lane_splat(na, r0 + 8 + m) for m in range(8)]
            na = jnp.where(inside, 0.0, na)
        rs, us, ums, done = [], [], [], p
        for j in range(8):
            r = lax.rsqrt(row_splat(s[j], j))
            low = jnp.where(sub > j, s[j] * r, 0.0)
            um = {m: row_splat(s[m], j) * r for m in range(j + 1, 8)}
            for m in um:
                s[m] = s[m] - low * um[m]
            u = row_splat(p, j) * r
            p = p - low * u
            done = jnp.where(sub == j, u, done)
            if more:
                ln = nn[j] * r
                for m in um:
                    nn[m] = nn[m] - ln * um[m]
                na = na - ln * u
                for m in range(8):
                    nx[m] = nx[m] - ln * row_splat(ln, m)
            rs.append(r), us.append(u), ums.append(um)
        out[r0 : r0 + 8, :] = jnp.where(lane < r0 + 8, done, 0.0)
        for g in range(t + 2, NB // 8):
            rows = slice(8 * g, 8 * g + 8)
            wa = w[rows, :]
            sg = [lane_splat(wa, r0 + j) for j in range(8)]
            wa = jnp.where(inside, 0.0, wa)
            for j in range(8):
                low = sg[j] * rs[j]
                for m in range(j + 1, 8):
                    sg[m] = sg[m] - low * ums[j][m]
                wa = wa - low * us[j]
            w[rows, :] = wa
        if more:
            p, s = na, nx


def dot6(a3, b3, dims):
    ca, cb = dims[0][0][0], dims[0][1][0]
    ah, am, al = a3
    bh, bm, bl = b3
    left = jnp.concatenate([ah, ah, am, ah, al, am], axis=ca)
    right = jnp.concatenate([bh, bm, bh, bl, bh, bm], axis=cb)
    return mm(left, right, dims)


def invert_factor(z, w, m11, m, midway, after):
    eye = jnp.where(
        lax.broadcasted_iota(jnp.int32, (NB, NB), 0) == lax.broadcasted_iota(jnp.int32, (NB, NB), 1), 1.0, 0.0
    ).astype(F32)
    cols = lax.broadcasted_iota(jnp.int32, (NB, K), 1)
    wide = lax.broadcasted_iota(jnp.int32, (K, K), 1)

    def block_step(kb, carry):
        c0 = pl.multiple_of(kb * NB, NB)
        c1 = c0 + NB
        rows = pl.ds(c0, NB)
        w[...] = z[rows, rows]
        eliminate_block(w, m11, lambda: midway(kb))
        z[rows, rows] = eye
        t = dot6(split3(m11[...]), split3(z[rows, :]), NN)
        m[rows, :] = jnp.where(cols < c1, t, 0.0)
        after(kb)

        @pl.when(kb < K // NB - 1)
        def _():
            update = dot6(split3(jnp.where(cols >= c1, t, 0.0)), split3(t), T0)
            z[...] = jnp.where((wide >= c0) & (wide < c1), 0.0, z[...]) - update

        return carry

    lax.fori_loop(0, K // NB, block_step, 0)


def finish_kernel(scale, m_ref, c_ref, modes_ref, red_ref, out_ref, z, sem):
    copy = pltpu.make_async_copy(modes_ref, out_ref, sem)
    copy.start()
    unpack(z, c_ref, 2)
    hi, lo = split2(m_ref[...])
    ch, cl = split2(z[...])
    for n, k1 in ((0, 256), (256, 512)):
        h, l, ah, al = hi[n : n + 256, :k1], lo[n : n + 256, :k1], ch[:k1], cl[:k1]
        z[n : n + 256, :] = mm(h, ah, NN) + mm(h, al, NN) + mm(l, ah, NN)
    lh, ll = split2(z[...])
    for n, k1 in ((0, 256), (256, 512)):
        h, l, ah, al = hi[n : n + 256, :k1], lo[n : n + 256, :k1], lh[:, :k1], ll[:, :k1]
        red_ref[:, n : n + 256] = (mm(ah, h, NT) + mm(ah, l, NT) + mm(al, h, NT)) * scale
    copy.wait()


def finish(m, cross, modes, scale):
    in_vmem = pl.BlockSpec(memory_space=pltpu.VMEM)
    anywhere = pl.BlockSpec(memory_space=pl.ANY)
    return pl.pallas_call(
        functools.partial(finish_kernel, scale),
        out_shape=(jax.ShapeDtypeStruct((K, K), F32), jax.ShapeDtypeStruct(modes.shape, F32)),
        in_specs=[in_vmem, in_vmem, anywhere],
        out_specs=(in_vmem, anywhere),
        scratch_shapes=[pltpu.VMEM((K, K), F32), pltpu.SemaphoreType.DMA(())],
        compiler_params=pltpu.CompilerParams(vmem_limit_bytes=24 << 20),
        name="operator",
    )(m, cross, modes)


def place(ref, group, i, first, value):
    per = ref.shape[1] // NB
    for n in range(value.shape[1] // NB):
        b = GROUPS[group].index((i, first + n))
        ref[b // per, (b % per) * NB : (b % per + 1) * NB, :] = value[:, n * NB : (n + 1) * NB]


def unpack(z, ref, group):
    per = ref.shape[1] // NB
    for b, (i, j) in enumerate(GROUPS[group]):
        z[i * NB : (i + 1) * NB, j * NB : (j + 1) * NB] = ref[b // per, (b % per) * NB : (b % per + 1) * NB, :]


def sums_kernel(scale, x_hbm, y_hbm, m_out, c_out, mode_out, mh, ml, z, w, m11, xv, yv, xh, xl, yh, yl, g0_out, g1_out,
                loc0, loc1, loc2, other0, other1, other2, chip0, chip1, chip2, land0, land1, cland1, cland2, cpart, cown, mine0, mine1,
                lz0, lz1, lz2, in_sem, d_send, d_recv, xy_send, xy_recv, z_send, z_recv, ag_send, ag_recv, e_send, e_recv,
                c_send, c_recv, f_send, f_recv):
    my, mz, mc, mx = [lax.axis_index(a) for a in AXES]
    oc = 1 - mc
    me = my * 4 + mx
    chunks = xv.shape[0] // 256
    loc, other, chip, land = (loc0, loc1, loc2), (other0, other1, other2), (chip0, chip1, chip2), (land0, land1)
    out = (g0_out, g1_out)
    plane = [(dy, dx) for dy in range(4) for dx in range(4)][1:]

    loads = []
    for n, (src, dst) in enumerate(((x_hbm, xv), (y_hbm, yv))):
        for i in range(chunks):
            part = pl.ds(i * 256, 256)
            loads.append(pltpu.make_async_copy(src.at[part], dst.at[part], in_sem.at[n * chunks + i]))
    for load in loads:
        load.start()

    def in_plane(dy, dx):
        return lax.rem(my + dy + 4, 4), lax.rem(mx + dx + 4, 4)

    def along_z(dz):
        return lax.rem(mz + dz, 8)

    barrier = pltpu.get_barrier_semaphore()
    pl.semaphore_signal(barrier, inc=1, device_id=(my, mz, oc, mx), device_id_type=MESH)
    for dy, dx in plane:
        py, px = in_plane(dy, dx)
        pl.semaphore_signal(barrier, inc=1, device_id=(py, mz, mc, px), device_id_type=MESH)
    for dz in range(1, 8):
        pl.semaphore_signal(barrier, inc=1, device_id=(my, along_z(dz), mc, mx), device_id_type=MESH)

    def piece(ref, who, size):
        return ref.at[pl.ds(pl.multiple_of(who * size, 8), size), :]

    def to_partner(src, dst, sends, recvs):
        return pltpu.make_async_remote_copy(src, dst, sends, recvs, device_id=(my, mz, oc, mx), device_id_type=MESH)

    def to_plane(src, dst, k, sends, recvs):
        py, px = in_plane(*plane[k])
        return pltpu.make_async_remote_copy(src, dst, sends, recvs, device_id=(py, mz, mc, px), device_id_type=MESH)

    def to_z(src, dst, k, sends, recvs):
        return pltpu.make_async_remote_copy(src, dst, sends, recvs, device_id=(my, along_z(k + 1), mc, mx), device_id_type=MESH)

    def start(copies):
        for c in copies:
            c.start()
        return copies

    def wait(copies):
        for c in copies:
            c.wait()

    def pair(n):
        return start([to_partner(loc[n].at[oc], other[n], d_send.at[n], d_recv.at[n])])

    def scatter(n, copies):
        wait(copies)
        chip[n][...] = loc[n][mc] + other[n][...]
        made = []
        for k in range(15):
            py, px = in_plane(*plane[k])
            made.append(to_plane(piece(chip[n], py * 4 + px, PIECE[n]), land[n].at[k], k, xy_send.at[n, k], xy_recv.at[n, k]))
        return start(made)

    def plane_sum(n, copies):
        wait(copies)
        total = chip[n][pl.ds(pl.multiple_of(me * PIECE[n], 8), PIECE[n]), :]
        for k in range(15):
            total = total + land[n][k]
        return total

    def spread_z(n, copies):
        mine, lz = ((mine0, lz0), (mine1, lz1))[n]
        total = plane_sum(n, copies)
        mine[...] = total
        lz[mz] = total
        return start([to_z(mine, lz.at[mz], k, z_send.at[n, k], z_recv.at[n, k]) for k in range(7)])

    def gather_plane(n):
        mine = piece(out[n].at[mc], me, PIECE[n])
        made = start([to_plane(mine, mine, k, ag_send.at[n, k], ag_recv.at[n, k]) for k in range(15)])
        return made, start([to_partner(mine, mine, e_send.at[n, 15], e_recv.at[n, 15])])

    def gather(n, copies):
        lz = (lz0, lz1)[n]
        wait(copies)
        total = lz[0]
        for k in range(1, 8):
            total = total + lz[k]
        out[n][mc, pl.ds(pl.multiple_of(me * PIECE[n], 8), PIECE[n]), :] = total
        return gather_plane(n)

    def pass_on(n, state):
        made, sent = state
        for k, (dy, dx) in enumerate(plane):
            made[k].wait_recv()
            py, px = in_plane(-dy, -dx)
            landed = piece(out[n].at[mc], py * 4 + px, PIECE[n])
            sent = sent + start([to_partner(landed, landed, e_send.at[n, k], e_recv.at[n, k])])
        for c in made:
            c.wait_send()
        return sent

    a_rows = lambda x, y: x * NB + y * 32
    b_rows = lambda y, x: HALF[2] // 2 + y * NB + x * 32

    def line(half, along_x, d):
        return (my, mz, mc, lax.rem(mx + d + 4, 4)) if along_x else (lax.rem(my + d + 4, 4), mz, mc, mx)

    def on_line(stage, half, along_x, d, src, dst):
        return pltpu.make_async_remote_copy(src, dst, c_send.at[stage, half, d - 1], c_recv.at[stage, half, d - 1],
                                            device_id=line(half, along_x, d), device_id_type=MESH)

    def aligned(ref, first, size):
        return ref.at[pl.ds(pl.multiple_of(first, 8), size), :]

    def cross_first(copies):
        wait(copies)
        chip2[...] = loc2[mc] + other2[...]
        made = []
        for d in (1, 2, 3):
            made.append(on_line(0, 0, True, d, aligned(chip2, a_rows(lax.rem(mx + d, 4), 0), NB), cland1.at[0, d - 1]))
            made.append(on_line(0, 1, False, d, aligned(chip2, b_rows(lax.rem(my + d, 4), 0), NB), cland1.at[1, d - 1]))
        return start(made)

    def cross_second(copies):
        wait(copies)
        for half, first in ((0, a_rows(mx, 0)), (1, b_rows(my, 0))):
            cpart[half] = chip2[pl.ds(pl.multiple_of(first, 8), NB), :] + cland1[half, 0] + cland1[half, 1] + cland1[half, 2]
        made = []
        for d in (1, 2, 3):
            made.append(on_line(1, 0, False, d, aligned(cpart.at[0], lax.rem(my + d, 4) * 32, 32), cland2.at[0, d - 1]))
            made.append(on_line(1, 1, True, d, aligned(cpart.at[1], lax.rem(mx + d, 4) * 32, 32), cland2.at[1, d - 1]))
        return start(made)

    def cross_z(copies):
        wait(copies)
        for half, first in ((0, my * 32), (1, mx * 32)):
            cown[half * 32 : half * 32 + 32, :] = (
                cpart[half, pl.ds(pl.multiple_of(first, 8), 32), :] + cland2[half, 0] + cland2[half, 1] + cland2[half, 2]
            )

    upper = mz // 4
    own = pl.ds(pl.multiple_of((1 - upper) * a_rows(mx, my) + upper * b_rows(my, mx) + lax.rem(mz, 4) * 8, 8), 8)

    def cross_back(copies):
        wait(copies)
        total = cown[pl.ds(pl.multiple_of(mz * 8, 8), 8), :]
        for k in range(7):
            total = total + lz2[k]
        c_out[mc, own, :] = total

    def cross_lines(stage, size, swap):
        made = []
        for d in (1, 2, 3):
            for half, first in ((0, a_rows(mx, 0 if swap else my)), (1, b_rows(my, 0 if swap else mx))):
                rows = aligned(c_out.at[mc], first, size)
                made.append(on_line(stage, half, (half == 0) == swap, d, rows, rows))
        return made

    def cross_forwards():
        made = [(0, a_rows(mx, 0)), (4, b_rows(my, 0))]
        for d in (1, 2, 3):
            made += [(d, a_rows(lax.rem(mx - d + 4, 4), 0)), (4 + d, b_rows(lax.rem(my - d + 4, 4), 0))]
        return [to_partner(aligned(c_out.at[mc], first, NB), aligned(c_out.at[mc], first, NB), f_send.at[k], f_recv.at[k])
                for k, first in made]

    for i in range(chunks):
        loads[i].wait()
        part = slice(i * 256, i * 256 + 256)
        xh[part, :], xl[part, :] = split2(xv[part, :])

    def gram_band(c0, c1):
        h, l, h2, l2 = xh[:, c0:c1], xl[:, c0:c1], xh[:, c0:], xl[:, c0:]
        return mm(h, h2, T0) + mm(h, l2, T0) + mm(l, h2, T0) + mm(l, l2, T0)

    place(loc0, 0, 0, 0, gram_band(0, NB))
    pl.semaphore_wait(barrier, 1 + len(plane) + 7)
    g0 = pair(0)
    place(loc1, 1, 1, 1, gram_band(NB, 2 * NB))
    g = gram_band(2 * NB, K)
    place(loc1, 1, 2, 2, g[:NB])
    place(loc1, 1, 3, 3, g[NB:, NB:])
    g1 = pair(1)
    g0 = scatter(0, g0)
    for i in range(chunks):
        loads[chunks + i].wait()
        part = slice(i * 256, i * 256 + 256)
        yh[part, :], yl[part, :] = split2(yv[part, :])
    g1 = scatter(1, g1)
    def cross_half(half):
        for i in range(2):
            band = pl.ds(pl.multiple_of((half * 2 + i) * NB, NB), NB)
            h, l = xh[:, band], xl[:, band]
            value = mm(h, yh[...], T0) + mm(h, yl[...], T0) + mm(l, yh[...], T0)
            for j in range(4):
                loc2[half, (4 * i + j) * NB : (4 * i + j + 1) * NB, :] = value[:, j * NB : (j + 1) * NB]

    cross_half(oc)
    c = pair(2)
    g0 = spread_z(0, g0)
    cross_half(mc)
    c = cross_first(c)
    g1 = spread_z(1, g1)
    g0 = gather(0, g0)
    c = cross_second(c)
    g1 = gather(1, g1)
    g0 = pass_on(0, g0)
    c_over = [to_z(piece(cown, along_z(k + 1), 8), lz2.at[k], k, z_send.at[2, k], z_recv.at[2, k]) for k in range(7)]
    c_rows = c_out.at[mc, own, :]
    c_back = [to_z(c_rows, c_rows, k, z_send.at[3, k], z_recv.at[3, k]) for k in range(7)]
    c_third = cross_lines(2, 32, False)
    c_fourth = cross_lines(3, NB, True)
    c_sent = cross_forwards()

    def awaited(n):
        copies = []
        for k, (dy, dx) in enumerate(plane):
            py, px = in_plane(-dy, -dx)
            landed = piece(out[n].at[mc], py * 4 + px, PIECE[n])
            copies.append(to_partner(landed, landed, e_send.at[n, k], e_recv.at[n, k]))
        mine = piece(out[n].at[mc], me, PIECE[n])
        return copies + [to_partner(mine, mine, e_send.at[n, 15], e_recv.at[n, 15])]

    def midway(kb):
        @pl.when(kb == 0)
        def _():
            pass_on(1, g1)

        @pl.when(kb == 2)
        def _():
            wait(c_back)
            start(c_third)

        @pl.when(kb == 3)
        def _():
            wait(c_third)
            start(c_fourth)
            start(c_sent[:2])

    def after(kb):
        @pl.when(kb == 0)
        def _():
            wait(awaited(1))
            unpack(z, g1_out, 1)
            cross_back(c_over)
            start(c_back)

    cross_z(c)
    start(c_over)
    wait(g0)
    unpack(z, g0_out, 0)
    invert_factor(z, w, m11, m_out, midway, after)

    mh[...], ml[...] = split2(m_out[...])

    def modes(i, carry):
        rows = pl.ds(pl.multiple_of(i * 256, 256), 256)
        for n, k1 in ((0, 256), (256, 512)):
            ph, plo = mh[n : n + 256, :k1], ml[n : n + 256, :k1]
            ah, al = yh[rows, :k1], yl[rows, :k1]
            mode_out[rows, n : n + 256] = (mm(ah, ph, NT) + mm(ah, plo, NT) + mm(al, ph, NT)) * scale

        @pl.when(i == 4)
        def _():
            for k, copy in enumerate(c_fourth):
                copy.wait_recv()
                c_sent[2 + k].start()
            for copy in c_fourth:
                copy.wait_send()

        return carry

    lax.fori_loop(0, chunks, modes, 0)
    wait(c_sent)


def sums(x, y, scale):
    rows = x.shape[0]
    vm = pltpu.VMEM
    dma = pltpu.SemaphoreType.DMA
    per_group = lambda lead, sizes: [vm((*lead, size, NB), F32) for size in sizes]
    return pl.pallas_call(
        functools.partial(sums_kernel, scale),
        out_shape=(
            jax.ShapeDtypeStruct((K, K), F32),
            jax.ShapeDtypeStruct((2, HALF[2], NB), F32),
            jax.ShapeDtypeStruct((rows, K), F32),
        ),
        in_specs=[pl.BlockSpec(memory_space=pltpu.MemorySpace.HBM)] * 2,
        out_specs=(pl.BlockSpec(memory_space=pltpu.VMEM),) * 3,
        scratch_shapes=[
            vm((K, K), BF16), vm((K, K), BF16),
            vm((K, K), F32), vm((NB, NB), F32), vm((NB, NB), F32),
            vm((rows, K), F32), vm((rows, K), F32),
            vm((rows, K), BF16), vm((rows, K), BF16), vm((rows, K), BF16), vm((rows, K), BF16),
            *per_group((2,), HALF[:2]),
            *per_group((2,), HALF), *per_group((), HALF), *per_group((), HALF), *per_group((15,), PIECE[:2]),
            vm((2, 3, NB, NB), F32), vm((2, 3, 32, NB), F32), vm((2, NB, NB), F32), vm((64, NB), F32),
            *per_group((), PIECE[:2]), *per_group((8,), PIECE[:2]), vm((7, 8, NB), F32),
            dma((2 * (rows // 256),)), dma((3,)), dma((3,)), dma((2, 15)), dma((2, 15)), dma((4, 7)), dma((4, 7)),
            dma((2, 15)), dma((2, 15)), dma((2, 16)), dma((2, 16)), dma((4, 2, 3)), dma((4, 2, 3)), dma((8,)), dma((8,)),
        ],
        compiler_params=pltpu.CompilerParams(collective_id=0, has_side_effects=True, vmem_limit_bytes=32 << 20),
        name="sums_and_factor",
    )(x, y)


def on_device(first_snaps, next_snaps):
    scale = math.sqrt(first_snaps.shape[0] * lax.axis_size(AXES))
    hbm = pltpu.MemorySpace.HBM
    in_hbm = [pltpu.with_memory_space_constraint(a, hbm) for a in (first_snaps, next_snaps)]
    inverse, cross, modes = sums(*in_hbm, scale)
    return finish(inverse, cross, modes, scale)


def solution(mesh):
    finer = Mesh(mesh.devices.reshape(4, 8, 2, 4), AXES)
    spec = P(AXES, None)
    return jax.shard_map(
        on_device, mesh=finer, in_specs=(spec, spec), out_specs=(P(), spec), check_vma=False
    )
```
